32 devices in a mesh: task: 8 (over z, y), occ: 4 (over x, core).
Axes of the slice: x: 2, y: 2, z: 4, core: 2. Of those that a mesh axis runs over, the one named last changes fastest.
Arguments:
- ao_tiles: bfloat16 [1280, 8, 32, 128], P('task'), may hold values from -6 to 6
- mo_coeffs: bfloat16 [1536, 200], P(None, 'occ'), may hold values from -0.5 to 0.5
- mu_blocks: int32 [1280], P('task'), may hold values from 0 to 191
- nu_blocks: int32 [1280], P('task'), may hold values from 0 to 47
- tile_live: int32 [1280], P('task'), may hold values 0 or 1
- batch_target: int32 [160], P('task'), may hold values from 0 to 2
- batch_count: int32 [8], P('task'), may hold values from 1 to 20
Outputs:
- half_mo: float32 [200, 200, 1024], P('occ', None, 'task')
The draws below stay inside these ranges and needn't reach their ends.
Inputs may be any that keep to these rules, and one draw needn't show every extreme that they name: `batch_target`: the batch's kl block is the block owned by task index (own index + value) mod 8. `batch_count`: batches at or after this count in a list are not part of the work.
All inputs are finite; a program needn't handle non-finite values. No bound on the sum of `tile_live` on one device may be relied on, other than what follows from the above.
Results may differ from the reference program's by a relative error of at most 0.0029.
Values may be sent and summed in bfloat16 or wider, within the bound.
A program may use at most 128 MiB of HBM per device.

```python
import jax
import jax.numpy as jnp
from jax import lax

NBF = 1536
NOCC = 200
MUT = 8
NUT = 32
KLW = 128
BATCH = 8
NB = 20
SPREAD = 3
BLOCKS = 160
TILES = 1280
N_TASK = 8


def with_ends(result, rng, smallest, largest):
    index_at = [jax.random.randint(jax.random.fold_in(rng, axis), (), 0, length) for axis, length in enumerate(result.shape)]
    widest = result.shape.index(max(result.shape))
    neighbour = index_at[:widest] + [(index_at[widest] + 1) % result.shape[widest]] + index_at[widest + 1:]
    return result.at[tuple(index_at)].set(smallest).at[tuple(neighbour)].set(largest)


def steps_of(own_key, shape, cuts, least, high):
    gain, own = 1.0, jax.random.fold_in(own_key, 6)
    for dim, shards_of in cuts:
        heights = jnp.exp(jax.random.uniform(jax.random.fold_in(own, dim), (shards_of,), jnp.float32, least / len(cuts), high / len(cuts)))
        gain = gain * jnp.repeat(heights, shape[dim] // shards_of).reshape([-1 if axis == dim else 1 for axis in range(len(shape))])
    return gain


def scatter_about(own_key, dims, spread, reach, split=(), held_as=jnp.bfloat16):
    level = steps_of(own_key, dims, split, -0.22, 0.18) if split else 1.0
    array = jax.random.normal(own_key, dims, jnp.float32) * spread * level
    return jnp.minimum(jnp.maximum(array, -reach), reach).astype(held_as)


def setup_inputs(seed: int = 0) -> dict:
    key_list = jax.random.split(jax.random.key(seed), 8)
    return {
        "ao_tiles": scatter_about(key_list[0], (TILES, MUT, NUT, KLW), 1.0, 6.0, ((0, 8),)),
        "mo_coeffs": scatter_about(key_list[1], (NBF, NOCC), 128 ** -0.5, 0.5, ((1, 4),)),
        "mu_blocks": with_ends(jax.random.randint(key_list[2], (TILES,), 0, NBF // MUT), jax.random.fold_in(key_list[2], 1), 0, (NBF // MUT) - 1).astype(jnp.int32),
        "nu_blocks": with_ends(jax.random.randint(key_list[3], (TILES,), 0, NBF // NUT), jax.random.fold_in(key_list[3], 1), 0, (NBF // NUT) - 1).astype(jnp.int32),
        "tile_live": with_ends((jax.random.randint(key_list[4], (TILES,), 0, 4) < 3).astype(jnp.int32), jax.random.fold_in(key_list[4], 1), 0, 1),
        "batch_target": with_ends(jax.random.randint(key_list[5], (BLOCKS,), 0, SPREAD), jax.random.fold_in(key_list[5], 1), 0, SPREAD - 1).astype(jnp.int32),
        "batch_count": with_ends(jax.random.randint(key_list[6], (N_TASK,), 1, NB + 1), jax.random.fold_in(key_list[6], 1), 1, NB).astype(jnp.int32),
    }


def reference(ao_tiles, mo_coeffs, mu_blocks, nu_blocks, tile_live, batch_target, batch_count):
    coeff_full = mo_coeffs.astype(jnp.float32)
    tiles_all = ao_tiles.reshape(N_TASK, NB, BATCH, MUT, NUT, KLW)
    mu_all = mu_blocks.reshape(N_TASK, NB, BATCH)
    nu_all = nu_blocks.reshape(N_TASK, NB, BATCH)
    live_all = tile_live.reshape(N_TASK, NB, BATCH)
    target_all = batch_target.reshape(N_TASK, NB)
    mu_offsets = jnp.arange(MUT, dtype=jnp.int32)
    nu_offsets = jnp.arange(NUT, dtype=jnp.int32)
    spread_ids = jnp.arange(SPREAD, dtype=jnp.int32)

    def one_group(output, group_items):
        tiles_g, mu_g, nu_g, live_g, target_g, listed, group_index = group_items

        def one_batch(partials, batch_items):
            tile_block, mu_ids, nu_ids, live_ids, target, batch_index = batch_items
            coeff_mu = coeff_full[mu_ids[:, None] * MUT + mu_offsets[None, :]]
            quarter = jnp.einsum("bmi,bmnk->bink", coeff_mu, tile_block.astype(jnp.float32)).astype(jnp.bfloat16)
            kept_tiles = (live_ids * (batch_index < listed).astype(jnp.int32)).astype(jnp.float32)
            coeff_nu = coeff_full[nu_ids[:, None] * NUT + nu_offsets[None, :]] * kept_tiles[:, None, None]
            contribution = jnp.einsum("bnj,bink->ijk", coeff_nu, quarter.astype(jnp.float32))
            chosen = (spread_ids == target).astype(jnp.float32)
            return partials + chosen[:, None, None, None] * contribution[None], None

        initial = jnp.zeros((SPREAD, NOCC, NOCC, KLW), jnp.float32)
        partials = lax.scan(one_batch, initial, (tiles_g, mu_g, nu_g, live_g, target_g, jnp.arange(NB, dtype=jnp.int32)))[0]
        for spread_index in range(SPREAD):
            owner_index = (group_index + spread_index) % N_TASK
            column = (owner_index * KLW).astype(jnp.int32)
            earlier = lax.dynamic_slice_in_dim(output, column, KLW, 2)
            output = lax.dynamic_update_slice_in_dim(output, earlier + partials[spread_index], column, 2)
        return output, None

    output = jnp.zeros((NOCC, NOCC, N_TASK * KLW), jnp.float32)
    output = lax.scan(one_group, output, (tiles_all, mu_all, nu_all, live_all, target_all, batch_count, jnp.arange(N_TASK, dtype=jnp.int32)))[0]
    return output
```

```python
from functools import partial

import jax
import jax.numpy as jnp
import numpy as np
from jax import lax
from jax.experimental import pallas as pl
from jax.experimental.pallas import tpu as pltpu
from jax.sharding import PartitionSpec as P

SPREAD = 3
GROUP = 8
LANES = 128
STEP = 2
F32 = jnp.float32
BF16 = jnp.bfloat16
MESH = pl.DeviceIdType.MESH


def up(value, unit):
    return -(-value // unit) * unit


def list_room(tiles):
    return up(tiles + 1, LANES)


def meta_rows(tiles):
    return up(SPREAD * list_room(tiles) // LANES + 1, 8)


def plan_kernel(occs, nu_range, live_ref, target_ref, count_ref, mu_ref, nu_ref, tiles, meta_ref, slots_ref, packed, held, taken, put):
    per_batch = live_ref.shape[0] // target_ref.shape[0]
    room = list_room(live_ref.shape[0])
    counts_at = SPREAD * room
    rows = packed.shape[1]
    me = lax.axis_index("occ")

    def clear(k, carry):
        meta_ref[counts_at + k] = 0
        return carry

    lax.fori_loop(0, LANES, clear, 0)

    def take_batch(batch, carry):
        target = target_ref[batch]
        at = meta_ref[counts_at + target]
        for q in range(per_batch):
            tile = batch * per_batch + q
            slots_ref[target * room + at] = tile
            meta_ref[target * room + at] = mu_ref[tile] * nu_range + nu_ref[tile]
            at = at + live_ref[tile]
        meta_ref[counts_at + target] = at
        return carry

    lax.fori_loop(0, count_ref[0], take_batch, 0)

    def fetch(s, row):
        k = (s - 1) * rows + row
        return pltpu.make_async_copy(tiles.at[slots_ref[s * room + row * occs + me]], held.at[k], taken.at[k])

    def store(s, row):
        k = (s - 1) * rows + row
        return pltpu.make_async_copy(held.at[k], packed.at[s - 1, row], put.at[k])

    def share(s):
        return lax.div(meta_ref[counts_at + s] - me + (occs - 1), occs)

    def each(s, act):
        def body(row, carry):
            act(s, row)
            return carry

        lax.fori_loop(0, share(s), body, 0)

    def forward(s, row):
        fetch(s, row).wait()
        store(s, row).start()

    for s in range(1, SPREAD):
        each(s, lambda s, row: fetch(s, row).start())
    for s in range(1, SPREAD):
        each(s, forward)
    for s in range(1, SPREAD):
        each(s, lambda s, row: store(s, row).wait())


def make_plan(occs, rows, nu_range, ao_tiles, tile_live, batch_target, batch_count, mu_blocks, nu_blocks):
    smem = pl.BlockSpec(memory_space=pltpu.SMEM)
    anywhere = pl.BlockSpec(memory_space=pl.ANY)
    tiles = tile_live.shape[0]
    held = (SPREAD - 1) * rows
    return pl.pallas_call(
        partial(plan_kernel, occs, nu_range),
        out_shape=(
            jax.ShapeDtypeStruct((meta_rows(tiles) * LANES,), jnp.int32),
            jax.ShapeDtypeStruct((SPREAD * list_room(tiles),), jnp.int32),
            jax.ShapeDtypeStruct((SPREAD - 1, rows) + ao_tiles.shape[1:], ao_tiles.dtype),
        ),
        in_specs=[smem] * 5 + [anywhere],
        out_specs=(smem, smem, anywhere),
        scratch_shapes=[
            pltpu.VMEM((held,) + ao_tiles.shape[1:], ao_tiles.dtype),
            pltpu.SemaphoreType.DMA((held,)),
            pltpu.SemaphoreType.DMA((held,)),
        ],
        compiler_params=pltpu.CompilerParams(vmem_limit_bytes=32 * 1024 * 1024),
        name="plan",
    )(tile_live, batch_target, batch_count, mu_blocks, nu_blocks, ao_tiles)


class Place:
    def __init__(self, tasks, occs):
        self.tasks, self.occs, self.chips = tasks, occs, occs // 2
        self.task, self.me = lax.axis_index("task"), lax.axis_index("occ")
        self.chip, self.core = self.me // 2, self.me % 2

    def ahead(self, hops):
        return {"task": (self.task + hops) % self.tasks, "occ": self.me}

    def across_index(self, hops):
        return (self.chip + hops + self.chips) % self.chips * 2 + self.core

    def across(self, hops):
        return {"task": self.task, "occ": self.across_index(hops)}

    def sibling_index(self):
        return self.chip * 2 + 1 - self.core

    def sibling(self):
        return {"task": self.task, "occ": self.sibling_index()}

    def greet(self, hops):
        barrier = pltpu.get_barrier_semaphore()
        others = [self.ahead(h) for h in hops] + [self.across(h) for h in range(1, self.chips)] + [self.sibling()]
        for other in others:
            pl.semaphore_signal(barrier, inc=1, device_id=other, device_id_type=MESH)
        pl.semaphore_wait(barrier, len(others))


def send(src, dst, sems, device):
    return pltpu.make_async_remote_copy(
        src_ref=src, dst_ref=dst, send_sem=sems[0], recv_sem=sems[1], device_id=device, device_id_type=MESH
    )


def exchange_kernel(
    tasks, occs, counts_row, classes, meta, coeff, near, coeffs, picked, far, told, heard, over, overed, side, sided, kept
):
    place = Place(tasks, occs)
    place.greet(range(1, tasks))

    def tell(hops):
        dst = near.at[hops] if hops < SPREAD else far.at[hops - SPREAD]
        return send(meta, dst, (told.at[hops - 1], heard.at[hops - 1]), place.ahead(hops))

    def cross(hops):
        return send(coeff, coeffs.at[place.me], (over.at[hops - 1], overed.at[hops - 1]), place.across(hops))

    def aside(hops):
        owner = place.across_index(-hops)
        src = coeffs.at[owner] if hops else coeff
        return send(src, coeffs.at[owner], (side.at[hops], sided.at[hops]), place.sibling())

    for hops in range(1, tasks):
        tell(hops).start()
    for hops in range(1, place.chips):
        cross(hops).start()
    aside(0).start()
    own = pltpu.make_async_copy(coeff, coeffs.at[place.me], kept.at[0])
    own.start()
    mine = pltpu.make_async_copy(meta, near.at[0], kept.at[1])
    mine.start()
    for hops in range(1, place.chips):
        cross(hops).wait_recv()
        aside(hops).start()
    own.wait()
    mine.wait()
    for hops in range(1, tasks):
        tell(hops).wait()
    for hops in range(1, place.chips):
        cross(hops).wait_send()
    for hops in range(place.chips):
        aside(hops).wait()
    most = jnp.int32(0)
    lane = lax.broadcasted_iota(jnp.int32, (1, LANES), 1)
    moved = (lane >= 1) & (lane < SPREAD)
    for ref, count in ((near, SPREAD), (far, tasks - SPREAD)):
        for k in range(count):
            row = ref[k, counts_row : counts_row + 1, :]
            most = jnp.maximum(most, jnp.max(jnp.where(moved, row, 0)))
    index = jnp.int32(0)
    for rows in classes[:-1]:
        index = index + jnp.where(most > rows * occs, 1, 0)
    picked[0] = index


def exchange(tasks, occs, tiles, classes, meta, coeff):
    anywhere = pl.BlockSpec(memory_space=pl.ANY)
    vmem = pl.BlockSpec(memory_space=pltpu.VMEM)
    chips = occs // 2
    dma = pltpu.SemaphoreType.DMA
    return pl.pallas_call(
        partial(exchange_kernel, tasks, occs, SPREAD * list_room(tiles) // LANES, classes),
        out_shape=(
            jax.ShapeDtypeStruct((SPREAD,) + meta.shape, meta.dtype),
            jax.ShapeDtypeStruct((occs,) + coeff.shape, coeff.dtype),
            jax.ShapeDtypeStruct((1,), jnp.int32),
        ),
        in_specs=[anywhere, anywhere],
        out_specs=(vmem, anywhere, pl.BlockSpec(memory_space=pltpu.SMEM)),
        scratch_shapes=[
            pltpu.VMEM((tasks - SPREAD,) + meta.shape, meta.dtype),
            dma((tasks - 1,)),
            dma((tasks - 1,)),
            dma((chips,)),
            dma((chips,)),
            dma((chips,)),
            dma((chips,)),
            dma((2,)),
        ],
        compiler_params=pltpu.CompilerParams(collective_id=0, has_side_effects=True),
        name="exchange",
    )(meta, coeff)


def move_kernel(tasks, occs, chunks, step, packed, recv, on, oned, over, overed, side, sided):
    place = Place(tasks, occs)
    place.greet((1, 2, tasks - 1, tasks - 2))

    def onward(s, k):
        at = pl.ds(k * step, step)
        return send(
            packed.at[s, at], recv.at[s, place.me, at], (on.at[s, k], oned.at[s, k]), place.ahead(s + 1)
        )

    def cross(s, k, hops):
        block = recv.at[s, place.me, pl.ds(k * step, step)]
        return send(block, block, (over.at[s, k, hops - 1], overed.at[s, k, hops - 1]), place.across(hops))

    def aside(s, k, hops):
        block = recv.at[s, place.across_index(-hops), pl.ds(k * step, step)]
        return send(block, block, (side.at[s, k, hops], sided.at[s, k, hops]), place.sibling())

    lists = range(SPREAD - 1)
    hopses = range(1, place.chips)

    def loop(lower, upper, act):
        def body(k, carry):
            act(k)
            return carry

        lax.fori_loop(lower, upper, body, 0)

    def launch(k):
        for s in lists:
            onward(s, k).start()

    def spread(k):
        for s in lists:
            onward(s, k).wait_recv()
            for hops in hopses:
                cross(s, k, hops).start()
            aside(s, k, 0).start()

    def relay(k):
        for s in lists:
            for hops in hopses:
                cross(s, k, hops).wait_recv()
                aside(s, k, hops).start()

    def both(k):
        spread(k)
        relay(k - 1)

    def finish(k):
        for s in lists:
            onward(s, k).wait_send()
            for hops in hopses:
                cross(s, k, hops).wait_send()
            for hops in range(place.chips):
                aside(s, k, hops).wait()

    loop(0, chunks, launch)
    spread(0)
    loop(1, chunks, both)
    relay(chunks - 1)
    loop(0, chunks, finish)


def move(tasks, occs, index, rows, step, packed):
    anywhere = pl.BlockSpec(memory_space=pl.ANY)
    chips = occs // 2
    chunks = rows // step
    dma = pltpu.SemaphoreType.DMA
    lists, total = packed.shape[:2]
    return pl.pallas_call(
        partial(move_kernel, tasks, occs, chunks, step),
        out_shape=jax.ShapeDtypeStruct((lists, occs, total) + packed.shape[2:], packed.dtype),
        in_specs=[anywhere],
        out_specs=anywhere,
        scratch_shapes=[
            dma((lists, chunks)),
            dma((lists, chunks)),
            dma((lists, chunks, chips)),
            dma((lists, chunks, chips)),
            dma((lists, chunks, chips)),
            dma((lists, chunks, chips)),
        ],
        compiler_params=pltpu.CompilerParams(collective_id=1 + index, has_side_effects=True),
        name="move" + str(rows),
    )(packed)


def contract_kernel(occs, nu_range, near_ref, slots_ref, tiles, moved, mine, coeffs, pick, own, interleave, unit, total, *refs):
    held, turned, quarter, coeff_i, coeff_all, address, code, landed = refs
    count, mu_width, nu_width, kl = tiles.shape
    occ, all_occ = total.shape[:2]
    depth = GROUP * mu_width
    across = (((1,), (1,)), ((), ()))
    turn = (((0,), (0,)), ((), ()))
    room = list_room(count)
    meta = near_ref.shape[0] // SPREAD
    share = moved.shape[0] // ((SPREAD - 1) * occs)

    coeff_i[...] = lax.dot_general(mine[...], unit[:occ, :occ], turn, preferred_element_type=F32)
    gathered = jnp.zeros(coeff_all.shape, F32)
    for q in range(occs):
        gathered += lax.dot_general(
            coeffs[q], unit[q * occ : (q + 1) * occ, :], turn, preferred_element_type=F32
        )
    coeff_all[...] = gathered

    filled = jnp.int32(0)
    for s in range(SPREAD):
        base = s * meta + s * room

        def note(p, at, s=s, base=base):
            if s == 0:
                place = slots_ref[p]
            else:
                place = count + ((s - 1) * occs + lax.rem(p, occs)) * share + lax.div(p, occs)
            address[at] = place
            code[at] = near_ref[base + p]
            return at + 1

        filled = lax.fori_loop(0, near_ref[s * meta + SPREAD * room + s], note, filled)
    for b in range(GROUP):
        address[filled + b] = 0
        code[filled + b] = 0
    groups = lax.div(filled + (GROUP - 1), GROUP)

    def start(group, slot):
        for b in range(GROUP):
            at = address[group * GROUP + b]

            @pl.when(at < count)
            def _():
                pltpu.make_async_copy(tiles.at[at], held.at[slot, b], landed.at[slot, b]).start()

            @pl.when(at >= count)
            def _():
                pltpu.make_async_copy(moved.at[at - count], held.at[slot, b], landed.at[slot, b]).start()

    def visit(group, slot):
        for b in range(GROUP):
            pltpu.make_async_copy(tiles.at[0], held.at[slot, b], landed.at[slot, b]).wait()

        @pl.when(group + 1 < groups)
        def _():
            start(group + 1, 1 - slot)

        for b in range(GROUP):
            for m in range(mu_width):
                turned[pl.ds(b * mu_width + m, nu_width, stride=depth), :] = held[slot, b, m].astype(F32)

        mus, nus = [], []
        for b in range(GROUP):
            place = group * GROUP + b
            both = code[place]
            mu, nu = lax.div(both, nu_range), lax.rem(both, nu_range)
            mus.append(coeff_i[pl.ds(pl.multiple_of(mu * mu_width, mu_width), mu_width), :])
            rows = coeff_all[pl.ds(pl.multiple_of(nu * nu_width, nu_width), nu_width), :]
            nus.append(rows * jnp.where(place < filled, 1.0, 0.0))
        mu_rows = jnp.concatenate(mus, axis=0).astype(BF16)
        nu_rows = jnp.concatenate(nus, axis=0).astype(BF16)
        left = lax.dot_general(pick[...], mu_rows, across, preferred_element_type=F32)
        left = (left * own[...]).astype(BF16)
        mixed = jnp.dot(interleave[...], nu_rows, preferred_element_type=F32).astype(BF16)
        right = lax.dot_general(unit[...], mixed, across, preferred_element_type=F32).astype(BF16)

        for p in range(nu_width // 2):
            even, later = 2 * p * depth, (2 * p + 1) * depth
            pair = jnp.concatenate(
                [turned[even : even + depth, :], turned[later : later + depth, :]], axis=1
            ).astype(BF16)
            got = jnp.dot(left, pair, preferred_element_type=F32).reshape(occ, GROUP, 2 * kl)
            got = jnp.concatenate([got[:, :, :kl], got[:, :, kl:]], axis=1)
            quarter[:, 2 * p * GROUP : (2 * p + 2) * GROUP, :] = got.astype(BF16)

        for h in range(occ // 2):
            both = jnp.concatenate([quarter[2 * h], quarter[2 * h + 1]], axis=1)
            got = jnp.dot(right, both, preferred_element_type=F32)
            total[2 * h] += got[:, :kl]
            total[2 * h + 1] += got[:, kl:]
        if occ % 2:
            total[occ - 1] += jnp.dot(right, quarter[occ - 1], preferred_element_type=F32)
        return 1 - slot

    total[...] = jnp.zeros_like(total)

    @pl.when(groups > 0)
    def _():
        start(0, 0)

    lax.fori_loop(0, groups, visit, jnp.int32(0))


def contract(nu_range, near, slots, ao_tiles, moved, mine, coeffs):
    count, mu_width, nu_width, kl = ao_tiles.shape
    occs, occ, basis = coeffs.shape
    all_occ = occs * occ
    depth, width = GROUP * mu_width, GROUP * nu_width
    moved = moved.reshape((-1,) + moved.shape[3:])

    def eq(rows, columns, dtype=BF16):
        return jnp.asarray(rows[:, None] == columns[None, :], dtype)

    out_rows = np.arange(occ * GROUP)
    pick = eq(out_rows // GROUP, np.arange(occ))
    own = eq(out_rows % GROUP, np.arange(depth) // mu_width, F32)
    mixed_rows = np.arange(width)
    interleave = eq(mixed_rows % GROUP * nu_width + mixed_rows // GROUP, mixed_rows)
    unit = eq(np.arange(all_occ), np.arange(all_occ))
    dense = [mine, coeffs, pick, own, interleave, unit]
    places = SPREAD * count + GROUP
    return pl.pallas_call(
        partial(contract_kernel, occs, nu_range),
        out_shape=jax.ShapeDtypeStruct((occ, all_occ, kl), F32),
        in_specs=[pl.BlockSpec(memory_space=pltpu.SMEM)] * 2
        + [pl.BlockSpec(memory_space=pl.ANY)] * 2
        + [pl.BlockSpec(memory_space=pltpu.VMEM)] * len(dense),
        out_specs=pl.BlockSpec(memory_space=pltpu.VMEM),
        scratch_shapes=[
            pltpu.VMEM((2, GROUP, mu_width, nu_width, kl), BF16),
            pltpu.VMEM((nu_width * depth, kl), F32),
            pltpu.VMEM((occ, width, kl), BF16),
            pltpu.VMEM((basis, occ), F32),
            pltpu.VMEM((basis, all_occ), F32),
            pltpu.SMEM((places,), jnp.int32),
            pltpu.SMEM((places,), jnp.int32),
            pltpu.SemaphoreType.DMA((2, GROUP)),
        ],
        compiler_params=pltpu.CompilerParams(vmem_limit_bytes=56 * 1024 * 1024),
        name="contract",
    )(near, slots, ao_tiles, moved, *dense)


def class_rows(rows):
    small = [r for r in (4, 8, 10, 12, 14, 16, 18, 20, 24) if r < rows]
    return small + [rows], [STEP] * len(small) + [max(STEP, rows // 10)]


def local(ao_tiles, mo_coeffs, mu_blocks, nu_blocks, tile_live, batch_target, batch_count):
    tiles, _, nu_width, _ = ao_tiles.shape
    tasks, occs = lax.axis_size("task"), lax.axis_size("occ")
    nu_range = mo_coeffs.shape[0] // nu_width
    rows = up(-(-tiles // occs), 10)
    classes, steps = class_rows(rows)
    coeff = mo_coeffs.T

    meta, slots, packed = make_plan(
        occs, rows, nu_range, ao_tiles, tile_live, batch_target, batch_count, mu_blocks, nu_blocks
    )
    near, coeffs, picked = exchange(tasks, occs, tiles, classes, meta.reshape(-1, LANES), coeff)
    branches = [
        partial(move, tasks, occs, index, size, step) for index, (size, step) in enumerate(zip(classes, steps))
    ]
    moved = lax.switch(picked[0], branches, packed)
    return contract(nu_range, near.reshape(-1), slots, ao_tiles, moved, coeff, coeffs)


def solution(mesh):
    in_specs = (
        P("task", None, None, None),
        P(None, "occ"),
        P("task"),
        P("task"),
        P("task"),
        P("task"),
        P("task"),
    )
    out_specs = P("occ", None, "task")
    return jax.shard_map(local, mesh=mesh, in_specs=in_specs, out_specs=out_specs, check_vma=False)
```

```python
from functools import partial

import jax
import jax.numpy as jnp
import numpy as np
from jax import lax
from jax.experimental import pallas as pl
from jax.experimental.pallas import tpu as pltpu
from jax.sharding import PartitionSpec as P

SPREAD = 3
GROUP = 8
LANES = 128
F32 = jnp.float32
BF16 = jnp.bfloat16
MESH = pl.DeviceIdType.MESH


def up(value, unit):
    return -(-value // unit) * unit


def list_room(tiles):
    return up(tiles + 1, LANES)


def meta_rows(tiles):
    return up(SPREAD * list_room(tiles) // LANES + 1, 8)


def plan_kernel(nu_range, live, target, count, mu, nu, meta_ref, slots_ref, live_ref, target_ref, count_ref, mu_ref, nu_ref, landed):
    sources = (live, target, count, mu, nu)
    held = (live_ref, target_ref, count_ref, mu_ref, nu_ref)
    copies = [pltpu.make_async_copy(src, dst, landed.at[k]) for k, (src, dst) in enumerate(zip(sources, held))]
    for copy in copies:
        copy.start()
    tiles = live_ref.shape[0]
    per_batch = tiles // target_ref.shape[0]
    room = list_room(tiles)
    counts_at = SPREAD * room
    unrolled = 8

    def clear(k, carry):
        for b in range(unrolled):
            meta_ref[counts_at + k * unrolled + b] = 0
        return carry

    def clear_lists(k, carry):
        for s in range(SPREAD):
            for b in range(unrolled):
                meta_ref[s * room + k * unrolled + b] = 0
                slots_ref[s * room + k * unrolled + b] = 0
        return carry

    lax.fori_loop(0, LANES // unrolled, clear, 0)
    lax.fori_loop(0, min(up(tiles, 2 * GROUP), room) // unrolled, clear_lists, 0)
    for copy in copies:
        copy.wait()

    def take_batch(batch, carry):
        target = target_ref[batch]
        at = meta_ref[counts_at + target]
        for q in range(per_batch):
            tile = batch * per_batch + q
            slots_ref[target * room + at] = tile
            meta_ref[target * room + at] = mu_ref[tile] * nu_range + nu_ref[tile]
            at = at + live_ref[tile]
        meta_ref[counts_at + target] = at
        return carry

    lax.fori_loop(0, count_ref[0], take_batch, 0)


def make_plan(nu_range, tile_live, batch_target, batch_count, mu_blocks, nu_blocks):
    smem = pl.BlockSpec(memory_space=pltpu.SMEM)
    tiles = tile_live.shape[0]
    ins = (tile_live, batch_target, batch_count, mu_blocks, nu_blocks)
    return pl.pallas_call(
        partial(plan_kernel, nu_range),
        out_shape=(
            jax.ShapeDtypeStruct((meta_rows(tiles) * LANES,), jnp.int32),
            jax.ShapeDtypeStruct((SPREAD * list_room(tiles),), jnp.int32),
        ),
        in_specs=[pl.BlockSpec(memory_space=pl.ANY)] * len(ins),
        out_specs=(smem, smem),
        scratch_shapes=[pltpu.SMEM(x.shape, jnp.int32) for x in ins] + [pltpu.SemaphoreType.DMA((len(ins),))],
        name="plan",
    )(*ins)


class Place:
    def __init__(self, tasks, occs):
        self.tasks, self.occs, self.chips = tasks, occs, occs // 2
        self.task, self.me = lax.axis_index("task"), lax.axis_index("occ")
        self.chip, self.core = self.me // 2, self.me % 2

    def ahead(self, hops):
        return {"task": (self.task + hops) % self.tasks, "occ": self.me}

    def across_index(self, hops):
        return (self.chip + hops + self.chips) % self.chips * 2 + self.core

    def across(self, hops):
        return {"task": self.task, "occ": self.across_index(hops)}

    def sibling_index(self):
        return self.chip * 2 + 1 - self.core

    def sibling(self):
        return {"task": self.task, "occ": self.sibling_index()}

    def greet(self, hops, inside=True):
        barrier = pltpu.get_barrier_semaphore()
        others = [self.ahead(h) for h in hops]
        if inside:
            others += [self.across(h) for h in range(1, self.chips)] + [self.sibling()]
        for other in others:
            pl.semaphore_signal(barrier, inc=1, device_id=other, device_id_type=MESH)
        pl.semaphore_wait(barrier, len(others))


def send(src, dst, sems, device):
    return pltpu.make_async_remote_copy(
        src_ref=src, dst_ref=dst, send_sem=sems[0], recv_sem=sems[1], device_id=device, device_id_type=MESH
    )


def exchange_kernel(tasks, occs, counts_row, classes, slots_ref, meta, tiles, near, packed, picked, far, held, told, heard, kept, taken):
    place = Place(tasks, occs)
    count = tiles.shape[0]
    parts = taken.shape[0]
    part = count // parts
    takes = [
        pltpu.make_async_copy(tiles.at[pl.ds(k * part, part)], held.at[pl.ds(k * part, part)], taken.at[k])
        for k in range(parts)
    ]
    for take in takes:
        take.start()
    mine = pltpu.make_async_copy(meta, near.at[0], kept)
    mine.start()
    place.greet(range(1, tasks), inside=False)

    def tell(hops):
        dst = near.at[hops] if hops < SPREAD else far.at[hops - SPREAD]
        return send(meta, dst, (told.at[hops - 1], heard.at[hops - 1]), place.ahead(hops))

    for hops in range(1, tasks):
        tell(hops).start()
    for take in takes:
        take.wait()
    room = list_room(count)

    def pack(row, carry):
        for s in range(1, SPREAD):
            packed[s - 1, row] = held[slots_ref[s * room + row * occs + place.me]]
        return carry

    lax.fori_loop(0, -(-count // occs), pack, 0)
    mine.wait()
    for hops in range(1, tasks):
        tell(hops).wait()
    most = jnp.int32(0)
    lane = lax.broadcasted_iota(jnp.int32, (1, LANES), 1)
    for ref, filled in ((near, SPREAD), (far, tasks - SPREAD)):
        for k in range(filled):
            row = ref[k, counts_row : counts_row + 1, :]
            most = jnp.maximum(most, jnp.max(jnp.where(lane < SPREAD, row, 0)))
    index = jnp.int32(0)
    for rows in classes[:-1]:
        index = index + jnp.where(most > rows * occs, 1, 0)
    picked[0] = index


def exchange(tasks, occs, rows, classes, slots, meta, ao_tiles):
    anywhere = pl.BlockSpec(memory_space=pl.ANY)
    vmem = pl.BlockSpec(memory_space=pltpu.VMEM)
    smem = pl.BlockSpec(memory_space=pltpu.SMEM)
    tiles = ao_tiles.shape[0]
    dma = pltpu.SemaphoreType.DMA
    return pl.pallas_call(
        partial(exchange_kernel, tasks, occs, SPREAD * list_room(tiles) // LANES, classes),
        out_shape=(
            jax.ShapeDtypeStruct((SPREAD,) + meta.shape, meta.dtype),
            jax.ShapeDtypeStruct((SPREAD - 1, rows) + ao_tiles.shape[1:], ao_tiles.dtype),
            jax.ShapeDtypeStruct((1,), jnp.int32),
        ),
        in_specs=[smem, anywhere, anywhere],
        out_specs=(vmem, vmem, smem),
        scratch_shapes=[
            pltpu.VMEM((tasks - SPREAD,) + meta.shape, meta.dtype),
            pltpu.VMEM(ao_tiles.shape, ao_tiles.dtype),
            dma((tasks - 1,)),
            dma((tasks - 1,)),
            dma,
            dma((8 if tiles % 8 == 0 else 1,)),
        ],
        compiler_params=pltpu.CompilerParams(
            collective_id=0, has_side_effects=True, vmem_limit_bytes=48 * 1024 * 1024
        ),
        name="exchange",
    )(slots, meta, ao_tiles)


def work_kernel(tasks, occs, nu_range, chunks, step, near_ref, slots_ref, tiles, packed, coeff, total, *refs):
    recv, held, coeffs, flat, spread_rows, coeff_i, left, lhs, stage, mixed, mu_rows = refs[:11]
    taken, kept, cover, covered, caside, casided, on, oned, over, overed, side, sided = refs[11:]
    place = Place(tasks, occs)
    count, mu_width, nu_width, kl = tiles.shape
    all_occ, occ = total.shape[:2]
    room = list_room(count)
    meta = near_ref.shape[0] // SPREAD
    counts_at = SPREAD * room
    per = LANES // nu_width
    lists = range(SPREAD - 1)
    hopses = range(1, place.chips)
    own_steps = (chunks + 1) // 2

    parts = taken.shape[0]
    part = count // parts
    takes = [
        pltpu.make_async_copy(tiles.at[pl.ds(k * part, part)], held.at[pl.ds(k * part, part)], taken.at[k])
        for k in range(parts)
    ]

    def coeff_cross(hops):
        return send(coeff, coeffs.at[place.me], (cover.at[hops - 1], covered.at[hops - 1]), place.across(hops))

    def coeff_aside(hops):
        owner = place.across_index(-hops)
        src = coeffs.at[owner] if hops else coeff
        return send(src, coeffs.at[owner], (caside.at[hops], casided.at[hops]), place.sibling())

    def onward(s, k):
        return send(
            packed.at[s, pl.ds(k * step, step)],
            recv.at[s, place.me, pl.ds(k * step, step)],
            (on.at[s, k], oned.at[s, k]),
            place.ahead(s + 1),
        )

    def cross(s, k, hops):
        block = recv.at[s, place.me, pl.ds(k * step, step)]
        return send(block, block, (over.at[s, k, hops - 1], overed.at[s, k, hops - 1]), place.across(hops))

    def aside(s, k, hops):
        block = recv.at[s, place.across_index(-hops), pl.ds(k * step, step)]
        return send(block, block, (side.at[s, k, hops], sided.at[s, k, hops]), place.sibling())

    def loop(upper, act):
        def body(k, carry):
            act(k)
            return carry

        lax.fori_loop(0, upper, body, 0)

    def launch(k):
        for s in lists:
            onward(s, k).start()

    def spread(k):
        for s in lists:
            onward(s, k).wait_recv()
            for hops in hopses:
                cross(s, k, hops).start()
            aside(s, k, 0).start()

    def relay(k):
        for s in lists:
            for hops in hopses:
                cross(s, k, hops).wait_recv()
                aside(s, k, hops).start()

    own_coeff = pltpu.make_async_copy(coeff, coeffs.at[place.me], kept)
    own_coeff.start()
    place.greet((1, 2, tasks - 1, tasks - 2))
    for hops in hopses:
        coeff_cross(hops).start()
    coeff_aside(0).start()
    loop(chunks, launch)
    for take in takes:
        take.start()
    total[...] = jnp.zeros_like(total)
    left[...] = jnp.zeros_like(left)
    for hops in hopses:
        coeff_cross(hops).wait_recv()
        coeff_aside(hops).start()
    own_coeff.wait()
    turn = (((0,), (0,)), ((), ()))

    def eye(rows):
        return (
            lax.broadcasted_iota(jnp.int32, (rows, rows), 0) == lax.broadcasted_iota(jnp.int32, (rows, rows), 1)
        ).astype(F32).astype(BF16)

    unit = eye(occ)
    rows_i = lax.dot_general(coeffs[place.me], unit, turn, preferred_element_type=F32)
    coeff_i[...] = rows_i.reshape(coeff_i.shape)
    for hops in range(place.chips):
        coeff_aside(hops).wait_recv()
    for q in range(occs):
        flat[q * occ : (q + 1) * occ, :] = coeffs[q].astype(F32)
    source = lax.broadcasted_iota(jnp.int32, (LANES, per * LANES), 0)
    column = lax.broadcasted_iota(jnp.int32, (LANES, per * LANES), 1)
    repeat = (source == column // LANES * nu_width + column % nu_width).astype(F32).astype(BF16)

    def lay(c, carry):
        block = flat[:, pl.ds(pl.multiple_of(c * LANES, LANES), LANES)].astype(BF16)
        got = jnp.dot(block, repeat, preferred_element_type=F32)
        for r in range(per):
            spread_rows[c * per + r] = got[:, r * LANES : (r + 1) * LANES]
        return carry

    lax.fori_loop(0, flat.shape[1] // LANES, lay, 0)
    for take in takes:
        take.wait()

    lane = lax.broadcasted_iota(jnp.int32, (1, LANES), 1) // nu_width
    band = all_occ // 4
    width = mu_width * GROUP

    def contract(base, valid):
        def first(g, carry):
            for b in range(GROUP):
                both = near_ref[(1 - g) * base[0] + g * base[1] + b]
                mu, nu = lax.div(both, nu_range), lax.rem(both, nu_range)
                live = jnp.where(b < (1 - g) * valid[0] + g * valid[1], 1.0, 0.0)
                mask = jnp.where(lane == b % per, live, 0.0)
                left[b // per, pl.ds(b, all_occ, stride=GROUP), :] = spread_rows[nu] * mask
                mu_rows[pl.ds(g * width + b, mu_width, stride=GROUP), :] = coeff_i[mu]
            for h in range(GROUP // per):
                lhs[:, h * LANES : (h + 1) * LANES] = left[h].astype(BF16)
            for p in range(mu_width // 2):
                halves = [
                    stage[pl.ds(g * GROUP, GROUP), m].reshape(GROUP * nu_width, kl) for m in (2 * p, 2 * p + 1)
                ]
                rhs = jnp.concatenate(halves, axis=1)
                for r in range(4):
                    got = jnp.dot(
                        lhs[r * band * GROUP : (r + 1) * band * GROUP, :], rhs, preferred_element_type=F32
                    ).reshape(band, GROUP, 2 * kl)
                    got = jnp.concatenate([got[:, :, :kl], got[:, :, kl:]], axis=1)
                    at = pl.ds(pl.multiple_of(g * width + 2 * p * GROUP, 2 * GROUP), 2 * GROUP)
                    mixed[r * band : (r + 1) * band, at, :] = got.astype(BF16)
            return carry

        lax.fori_loop(0, 2, first, 0)
        left_i = lax.dot_general(
            unit, mu_rows[...].astype(BF16), (((1,), (1,)), ((), ())), preferred_element_type=F32
        ).astype(BF16)
        pairs = 10 if all_occ % 20 == 0 else 1

        def second(h, carry):
            for d in range(pairs):
                j = 2 * (h * pairs + d)
                both = jnp.concatenate([mixed[j], mixed[j + 1]], axis=1)
                got = jnp.dot(left_i, both, preferred_element_type=F32)
                total[j] += got[:, :kl]
                total[j + 1] += got[:, kl:]
            return carry

        lax.fori_loop(0, all_occ // (2 * pairs), second, 0)

    def counted(s):
        return near_ref[s * meta + counts_at + s]

    far_off = chunks + 2 + own_steps

    def turn_of(k):
        @pl.when(k < chunks)
        def _():
            spread(k)

        @pl.when(k >= 1)
        def _():
            @pl.when(k <= chunks)
            def _():
                relay(k - 1)

        def one(j, carry):
            at = k * 2 * GROUP
            c = k - 2

            @pl.when(j == 0)
            def _():
                for b in range(2 * GROUP):
                    stage[b] = held[slots_ref[at + b]]

            @pl.when(j == 1)
            def _():
                for s in lists:
                    for hops in range(place.chips):
                        aside(s, c, hops).wait_recv()
                    for b in range(GROUP):
                        stage[s * GROUP + b] = recv[s, b % occs, c * step + b // occs]

            i = 1 - j
            base = (i * at + j * (meta + room + c * GROUP), i * (at + GROUP) + j * (2 * (meta + room) + c * GROUP))
            own = counted(0) - at
            valid = (i * own + j * (counted(1) - c * GROUP), i * (own - GROUP) + j * (counted(2) - c * GROUP))
            contract(base, valid)
            return carry

        lower = (k + far_off - own_steps) // far_off
        upper = 1 + (k + far_off - 2) // far_off
        lax.fori_loop(lower, upper, one, 0)

    loop(chunks + 2, turn_of)

    def finish(k):
        for s in lists:
            onward(s, k).wait_send()
            for hops in hopses:
                cross(s, k, hops).wait_send()
            for hops in range(place.chips):
                aside(s, k, hops).wait_send()

    loop(chunks, finish)
    for hops in hopses:
        coeff_cross(hops).wait_send()
    for hops in range(place.chips):
        coeff_aside(hops).wait_send()


def work(tasks, occs, nu_range, index, rows, step, near, slots, ao_tiles, packed, coeff):
    anywhere = pl.BlockSpec(memory_space=pl.ANY)
    smem = pl.BlockSpec(memory_space=pltpu.SMEM)
    vmem = pltpu.VMEM
    chips = occs // 2
    chunks = rows // step
    dma = pltpu.SemaphoreType.DMA
    lists = packed.shape[0]
    count, mu_width, nu_width, kl = ao_tiles.shape
    occ, basis = coeff.shape
    all_occ = occs * occ
    depth = 2 * GROUP * mu_width
    return pl.pallas_call(
        partial(work_kernel, tasks, occs, nu_range, chunks, step),
        out_shape=jax.ShapeDtypeStruct((all_occ, occ, kl), F32),
        in_specs=[smem, smem, anywhere, anywhere, anywhere],
        out_specs=pl.BlockSpec(memory_space=pltpu.VMEM),
        scratch_shapes=[
            vmem((lists, occs, rows) + packed.shape[2:], packed.dtype),
            vmem(ao_tiles.shape, ao_tiles.dtype),
            vmem((occs, occ, basis), BF16),
            vmem((all_occ, basis), F32),
            vmem((nu_range, all_occ, LANES), F32),
            vmem((basis // mu_width, mu_width, occ), F32),
            vmem((GROUP * nu_width // LANES, all_occ * GROUP, LANES), F32),
            vmem((all_occ * GROUP, GROUP * nu_width), BF16),
            vmem((2 * GROUP,) + ao_tiles.shape[1:], BF16),
            vmem((all_occ, depth, kl), BF16),
            vmem((depth, occ), F32),
            dma((8 if count % 8 == 0 else 1,)),
            dma,
            dma((chips,)),
            dma((chips,)),
            dma((chips,)),
            dma((chips,)),
            dma((lists, chunks)),
            dma((lists, chunks)),
            dma((lists, chunks, chips)),
            dma((lists, chunks, chips)),
            dma((lists, chunks, chips)),
            dma((lists, chunks, chips)),
        ],
        compiler_params=pltpu.CompilerParams(
            collective_id=1 + index, has_side_effects=True, vmem_limit_bytes=62 * 1024 * 1024
        ),
        name="work" + str(rows),
    )(near, slots, ao_tiles, packed, coeff)


CLASSES = (5, 6, 7, 8, 9, 10)


def local(ao_tiles, mo_coeffs, mu_blocks, nu_blocks, tile_live, batch_target, batch_count):
    tiles, _, nu_width, _ = ao_tiles.shape
    tasks, occs = lax.axis_size("task"), lax.axis_size("occ")
    nu_range = mo_coeffs.shape[0] // nu_width
    step = GROUP // occs
    rows = up(-(-tiles // occs), step)
    classes = [c * step for c in CLASSES if c * step < rows] + [rows]
    coeff = mo_coeffs.T

    meta, slots = make_plan(nu_range, tile_live, batch_target, batch_count, mu_blocks, nu_blocks)
    near, packed, picked = exchange(tasks, occs, rows, classes, slots, meta.reshape(-1, LANES), ao_tiles)
    branches = [partial(work, tasks, occs, nu_range, index, size, step) for index, size in enumerate(classes)]
    turned = lax.switch(picked[0], branches, near.reshape(-1), slots, ao_tiles, packed, coeff)
    return jnp.swapaxes(turned, 0, 1)


def solution(mesh):
    in_specs = (
        P("task", None, None, None),
        P(None, "occ"),
        P("task"),
        P("task"),
        P("task"),
        P("task"),
        P("task"),
    )
    out_specs = P("occ", None, "task")
    return jax.shard_map(local, mesh=mesh, in_specs=in_specs, out_specs=out_specs, check_vma=False)
```

```python
from functools import partial

import jax
import jax.numpy as jnp
import numpy as np
from jax import lax
from jax.experimental import pallas as pl
from jax.experimental.pallas import tpu as pltpu
from jax.sharding import PartitionSpec as P

SPREAD = 3
GROUP = 8
LANES = 128
F32 = jnp.float32
BF16 = jnp.bfloat16
MESH = pl.DeviceIdType.MESH


def up(value, unit):
    return -(-value // unit) * unit


def list_room(tiles):
    return up(tiles + 1, LANES)


def meta_rows(tiles):
    return up(SPREAD * list_room(tiles) // LANES + 1, 8)


def plan_kernel(nu_range, live, target, count, mu, nu, meta_ref, slots_ref, live_ref, target_ref, count_ref, mu_ref, nu_ref, landed):
    sources = (live, target, count, mu, nu)
    held = (live_ref, target_ref, count_ref, mu_ref, nu_ref)
    copies = [pltpu.make_async_copy(src, dst, landed.at[k]) for k, (src, dst) in enumerate(zip(sources, held))]
    for copy in copies:
        copy.start()
    tiles = live_ref.shape[0]
    per_batch = tiles // target_ref.shape[0]
    room = list_room(tiles)
    counts_at = SPREAD * room
    unrolled = 8

    def clear(k, carry):
        for b in range(unrolled):
            meta_ref[counts_at + k * unrolled + b] = 0
        return carry

    def clear_lists(k, carry):
        for s in range(SPREAD):
            for b in range(unrolled):
                meta_ref[s * room + k * unrolled + b] = 0
                slots_ref[s * room + k * unrolled + b] = 0
        return carry

    lax.fori_loop(0, LANES // unrolled, clear, 0)
    lax.fori_loop(0, min(up(tiles, 2 * GROUP) + 2 * GROUP, room) // unrolled, clear_lists, 0)
    for copy in copies:
        copy.wait()

    def take_batch(batch, carry):
        target = target_ref[batch]
        at = meta_ref[counts_at + target]
        for q in range(per_batch):
            tile = batch * per_batch + q
            slots_ref[target * room + at] = tile
            meta_ref[target * room + at] = mu_ref[tile] * nu_range + nu_ref[tile]
            at = at + live_ref[tile]
        meta_ref[counts_at + target] = at
        return carry

    lax.fori_loop(0, count_ref[0], take_batch, 0)


def make_plan(nu_range, tile_live, batch_target, batch_count, mu_blocks, nu_blocks):
    smem = pl.BlockSpec(memory_space=pltpu.SMEM)
    tiles = tile_live.shape[0]
    ins = (tile_live, batch_target, batch_count, mu_blocks, nu_blocks)
    return pl.pallas_call(
        partial(plan_kernel, nu_range),
        out_shape=(
            jax.ShapeDtypeStruct((meta_rows(tiles) * LANES,), jnp.int32),
            jax.ShapeDtypeStruct((SPREAD * list_room(tiles),), jnp.int32),
        ),
        in_specs=[pl.BlockSpec(memory_space=pl.ANY)] * len(ins),
        out_specs=(smem, smem),
        scratch_shapes=[pltpu.SMEM(x.shape, jnp.int32) for x in ins] + [pltpu.SemaphoreType.DMA((len(ins),))],
        name="plan",
    )(*ins)


class Place:
    def __init__(self, tasks, occs):
        self.tasks, self.occs, self.chips = tasks, occs, occs // 2
        self.task, self.me = lax.axis_index("task"), lax.axis_index("occ")
        self.chip, self.core = self.me // 2, self.me % 2

    def ahead(self, hops):
        return {"task": (self.task + hops) % self.tasks, "occ": self.me}

    def across_index(self, hops):
        return (self.chip + hops + self.chips) % self.chips * 2 + self.core

    def across(self, hops):
        return {"task": self.task, "occ": self.across_index(hops)}

    def sibling_index(self):
        return self.chip * 2 + 1 - self.core

    def sibling(self):
        return {"task": self.task, "occ": self.sibling_index()}

    def greet(self, hops, inside=True):
        barrier = pltpu.get_barrier_semaphore()
        others = [self.ahead(h) for h in hops]
        if inside:
            others += [self.across(h) for h in range(1, self.chips)] + [self.sibling()]
        for other in others:
            pl.semaphore_signal(barrier, inc=1, device_id=other, device_id_type=MESH)
        pl.semaphore_wait(barrier, len(others))


def send(src, dst, sems, device):
    return pltpu.make_async_remote_copy(
        src_ref=src, dst_ref=dst, send_sem=sems[0], recv_sem=sems[1], device_id=device, device_id_type=MESH
    )


def exchange_kernel(
    tasks, occs, counts_row, classes, slots_ref, meta, coeff, tiles, near, coeffs, packed, picked, *refs
):
    far, held, told, heard, over, overed, side, sided, kept, taken = refs
    place = Place(tasks, occs)
    count = tiles.shape[0]
    parts = taken.shape[0]
    part = count // parts
    takes = [
        pltpu.make_async_copy(tiles.at[pl.ds(k * part, part)], held.at[pl.ds(k * part, part)], taken.at[k])
        for k in range(parts)
    ]
    for take in takes:
        take.start()
    mine = pltpu.make_async_copy(meta, near.at[0], kept.at[0])
    mine.start()
    own = pltpu.make_async_copy(coeff, coeffs.at[place.me], kept.at[1])
    own.start()
    place.greet(range(1, tasks))

    def tell(hops):
        dst = near.at[hops] if hops < SPREAD else far.at[hops - SPREAD]
        return send(meta, dst, (told.at[hops - 1], heard.at[hops - 1]), place.ahead(hops))

    def cross(hops):
        return send(coeff, coeffs.at[place.me], (over.at[hops - 1], overed.at[hops - 1]), place.across(hops))

    def aside(hops):
        owner = place.across_index(-hops)
        src = coeffs.at[owner] if hops else coeff
        return send(src, coeffs.at[owner], (side.at[hops], sided.at[hops]), place.sibling())

    for hops in range(1, tasks):
        tell(hops).start()
    for hops in range(1, place.chips):
        cross(hops).start()
    aside(0).start()
    for take in takes:
        take.wait()
    room = list_room(count)

    def pack(row, carry):
        for s in range(1, SPREAD):
            packed[s - 1, row] = held[slots_ref[s * room + row * occs + place.me]]
        return carry

    lax.fori_loop(0, -(-count // occs), pack, 0)
    for hops in range(1, place.chips):
        cross(hops).wait_recv()
        aside(hops).start()
    mine.wait()
    own.wait()
    for hops in range(1, tasks):
        tell(hops).wait()
    most = jnp.int32(0)
    lane = lax.broadcasted_iota(jnp.int32, (1, LANES), 1)
    for ref, filled in ((near, SPREAD), (far, tasks - SPREAD)):
        for k in range(filled):
            row = ref[k, counts_row : counts_row + 1, :]
            most = jnp.maximum(most, jnp.max(jnp.where(lane < SPREAD, row, 0)))
    index = jnp.int32(0)
    for rows in classes[:-1]:
        index = index + jnp.where(most > rows * occs, 1, 0)
    picked[0] = index
    for hops in range(1, place.chips):
        cross(hops).wait_send()
    for hops in range(place.chips):
        aside(hops).wait()


def exchange(tasks, occs, rows, classes, slots, meta, coeff, ao_tiles):
    anywhere = pl.BlockSpec(memory_space=pl.ANY)
    vmem = pl.BlockSpec(memory_space=pltpu.VMEM)
    smem = pl.BlockSpec(memory_space=pltpu.SMEM)
    tiles = ao_tiles.shape[0]
    chips = occs // 2
    dma = pltpu.SemaphoreType.DMA
    return pl.pallas_call(
        partial(exchange_kernel, tasks, occs, SPREAD * list_room(tiles) // LANES, classes),
        out_shape=(
            jax.ShapeDtypeStruct((SPREAD,) + meta.shape, meta.dtype),
            jax.ShapeDtypeStruct((occs,) + coeff.shape, coeff.dtype),
            jax.ShapeDtypeStruct((SPREAD - 1, rows) + ao_tiles.shape[1:], ao_tiles.dtype),
            jax.ShapeDtypeStruct((1,), jnp.int32),
        ),
        in_specs=[smem, anywhere, anywhere, anywhere],
        out_specs=(vmem, anywhere, vmem, smem),
        scratch_shapes=[
            pltpu.VMEM((tasks - SPREAD,) + meta.shape, meta.dtype),
            pltpu.VMEM(ao_tiles.shape, ao_tiles.dtype),
            dma((tasks - 1,)),
            dma((tasks - 1,)),
            dma((chips,)),
            dma((chips,)),
            dma((chips,)),
            dma((chips,)),
            dma((2,)),
            dma((8 if tiles % 8 == 0 else 1,)),
        ],
        compiler_params=pltpu.CompilerParams(
            collective_id=0, has_side_effects=True, vmem_limit_bytes=48 * 1024 * 1024
        ),
        name="exchange",
    )(slots, meta, coeff, ao_tiles)


def work_kernel(tasks, occs, nu_range, chunks, step, near_ref, slots_ref, tiles, packed, coeffs, total, *refs):
    recv, held, flat, spread_rows, coeff_i, left_a, left_b, lhs_a, lhs_b, stage, mixed, mu_rows = refs[:12]
    taken, on, oned, over, overed, side, sided = refs[12:]
    place = Place(tasks, occs)
    count, mu_width, nu_width, kl = tiles.shape
    all_occ, occ = total.shape[:2]
    room = list_room(count)
    meta = near_ref.shape[0] // SPREAD
    counts_at = SPREAD * room
    per = LANES // nu_width
    lists = range(SPREAD - 1)
    hopses = range(1, place.chips)
    own_steps = (chunks + 1) // 2
    steps = own_steps + chunks

    parts = taken.shape[0]
    part = count // parts
    takes = [
        pltpu.make_async_copy(tiles.at[pl.ds(k * part, part)], held.at[pl.ds(k * part, part)], taken.at[k])
        for k in range(parts)
    ]

    def onward(s, k):
        return send(
            packed.at[s, pl.ds(k * step, step)],
            recv.at[s, place.me, pl.ds(k * step, step)],
            (on.at[s, k], oned.at[s, k]),
            place.ahead(s + 1),
        )

    def cross(s, k, hops):
        block = recv.at[s, place.me, pl.ds(k * step, step)]
        return send(block, block, (over.at[s, k, hops - 1], overed.at[s, k, hops - 1]), place.across(hops))

    def aside(s, k, hops):
        block = recv.at[s, place.across_index(-hops), pl.ds(k * step, step)]
        return send(block, block, (side.at[s, k, hops], sided.at[s, k, hops]), place.sibling())

    def loop(upper, act):
        def body(k, carry):
            act(k)
            return carry

        lax.fori_loop(0, upper, body, 0)

    def launch(k):
        for s in lists:
            onward(s, k).start()

    def spread(k):
        for s in lists:
            onward(s, k).wait_recv()
            for hops in hopses:
                cross(s, k, hops).start()
            aside(s, k, 0).start()

    def relay(k):
        for s in lists:
            for hops in hopses:
                cross(s, k, hops).wait_recv()
                aside(s, k, hops).start()

    for take in takes:
        take.start()
    place.greet((1, 2, tasks - 1, tasks - 2))
    loop(chunks, launch)
    total[...] = jnp.zeros_like(total)
    left_a[...] = jnp.zeros_like(left_a)
    left_b[...] = jnp.zeros_like(left_b)
    turn = (((0,), (0,)), ((), ()))
    unit = (
        lax.broadcasted_iota(jnp.int32, (occ, occ), 0) == lax.broadcasted_iota(jnp.int32, (occ, occ), 1)
    ).astype(F32).astype(BF16)
    rows_i = lax.dot_general(coeffs[place.me], unit, turn, preferred_element_type=F32)
    coeff_i[...] = rows_i.reshape(coeff_i.shape)
    for q in range(occs):
        flat[q * occ : (q + 1) * occ, :] = coeffs[q].astype(F32)
    source = lax.broadcasted_iota(jnp.int32, (LANES, per * LANES), 0)
    column = lax.broadcasted_iota(jnp.int32, (LANES, per * LANES), 1)
    repeat = (source == column // LANES * nu_width + column % nu_width).astype(F32).astype(BF16)

    def lay(c, carry):
        block = flat[:, pl.ds(pl.multiple_of(c * LANES, LANES), LANES)].astype(BF16)
        got = jnp.dot(block, repeat, preferred_element_type=F32)
        for r in range(per):
            spread_rows[c * per + r] = got[:, r * LANES : (r + 1) * LANES]
        return carry

    lax.fori_loop(0, flat.shape[1] // LANES, lay, 0)

    lane = lax.broadcasted_iota(jnp.int32, (1, LANES), 1) // nu_width
    band = all_occ // 4
    width = mu_width * GROUP
    far_off = steps + own_steps + 1

    def counted(s):
        return near_ref[s * meta + counts_at + s]

    def list_of(e, g):
        j = (e + far_off - own_steps) // far_off
        own, c = e * 2 * GROUP + g * GROUP, (e - own_steps) * GROUP
        base = (1 - j) * own + j * ((g + 1) * (meta + room) + c)
        return base, (1 - j) * (counted(0) - own) + j * (counted(g + 1) - c)

    def build(e, g, left, lhs):
        base, valid = list_of(e, g)
        for b in range(GROUP):
            live = jnp.where(b < valid, 1.0, 0.0)
            mask = jnp.where(lane == b % per, live, 0.0)
            nu = lax.rem(near_ref[base + b], nu_range)
            left[b // per, pl.ds(b, all_occ, stride=GROUP), :] = spread_rows[nu] * mask
        for h in range(GROUP // per):
            lhs[:, h * LANES : (h + 1) * LANES] = left[h].astype(BF16)

    def first(g, lhs):
        for p in range(mu_width // 2):
            halves = [stage[g * GROUP : (g + 1) * GROUP, m].reshape(GROUP * nu_width, kl) for m in (2 * p, 2 * p + 1)]
            rhs = jnp.concatenate(halves, axis=1)
            at = g * width + 2 * p * GROUP
            for r in range(4):
                got = jnp.dot(
                    lhs[r * band * GROUP : (r + 1) * band * GROUP, :], rhs, preferred_element_type=F32
                ).reshape(band, GROUP, 2 * kl)
                got = jnp.concatenate([got[:, :, :kl], got[:, :, kl:]], axis=1)
                mixed[r * band : (r + 1) * band, at : at + 2 * GROUP, :] = got.astype(BF16)

    def second(e):
        for g in range(2):
            base = list_of(e, g)[0]
            for b in range(GROUP):
                mu = lax.div(near_ref[base + b], nu_range)
                mu_rows[pl.ds(g * width + b, mu_width, stride=GROUP), :] = coeff_i[mu]
        left_i = lax.dot_general(
            unit, mu_rows[...].astype(BF16), (((1,), (1,)), ((), ())), preferred_element_type=F32
        ).astype(BF16)
        for j in range(0, all_occ, 2):
            both = jnp.concatenate([mixed[j], mixed[j + 1]], axis=1)
            got = jnp.dot(left_i, both, preferred_element_type=F32)
            total[j] += got[:, :kl]
            total[j + 1] += got[:, kl:]

    build(0, 0, left_a, lhs_a)
    for take in takes:
        take.wait()

    def take_step(e):
        @pl.when(e == 1)
        def _():
            spread(0)

        @pl.when(e == own_steps - 1)
        def _():
            spread(1)
            relay(0)

        c = e - own_steps

        @pl.when(e < own_steps)
        def _():
            for b in range(2 * GROUP):
                stage[b] = held[slots_ref[e * 2 * GROUP + b]]

        @pl.when(c >= 0)
        def _():
            @pl.when(c + 2 < chunks)
            def _():
                spread(c + 2)

            @pl.when(c + 1 < chunks)
            def _():
                relay(c + 1)

            for s in lists:
                for hops in range(place.chips):
                    aside(s, c, hops).wait_recv()
                for b in range(GROUP):
                    stage[s * GROUP + b] = recv[s, b % occs, c * step + b // occs]

        build(e, 1, left_b, lhs_b)
        first(0, lhs_a)
        first(1, lhs_b)
        build(e + 1, 0, left_a, lhs_a)
        second(e)

    loop(steps, take_step)

    def finish(k):
        for s in lists:
            onward(s, k).wait_send()
            for hops in hopses:
                cross(s, k, hops).wait_send()
            for hops in range(place.chips):
                aside(s, k, hops).wait_send()

    loop(chunks, finish)


def work(tasks, occs, nu_range, index, rows, step, near, slots, ao_tiles, packed, coeffs):
    anywhere = pl.BlockSpec(memory_space=pl.ANY)
    smem = pl.BlockSpec(memory_space=pltpu.SMEM)
    vmem = pltpu.VMEM
    chips = occs // 2
    chunks = rows // step
    dma = pltpu.SemaphoreType.DMA
    lists = packed.shape[0]
    count, mu_width, nu_width, kl = ao_tiles.shape
    _, occ, basis = coeffs.shape
    all_occ = occs * occ
    depth = 2 * GROUP * mu_width
    return pl.pallas_call(
        partial(work_kernel, tasks, occs, nu_range, chunks, step),
        out_shape=jax.ShapeDtypeStruct((all_occ, occ, kl), F32),
        in_specs=[smem, smem, anywhere, anywhere, pl.BlockSpec(memory_space=pltpu.VMEM)],
        out_specs=pl.BlockSpec(memory_space=pltpu.VMEM),
        scratch_shapes=[
            vmem((lists, occs, rows) + packed.shape[2:], packed.dtype),
            vmem(ao_tiles.shape, ao_tiles.dtype),
            vmem((all_occ, basis), F32),
            vmem((nu_range, all_occ, LANES), F32),
            vmem((basis // mu_width, mu_width, occ), F32),
            vmem((GROUP * nu_width // LANES, all_occ * GROUP, LANES), F32),
            vmem((GROUP * nu_width // LANES, all_occ * GROUP, LANES), F32),
            vmem((all_occ * GROUP, GROUP * nu_width), BF16),
            vmem((all_occ * GROUP, GROUP * nu_width), BF16),
            vmem((2 * GROUP,) + ao_tiles.shape[1:], BF16),
            vmem((all_occ, depth, kl), BF16),
            vmem((depth, occ), F32),
            dma((8 if count % 8 == 0 else 1,)),
            dma((lists, chunks)),
            dma((lists, chunks)),
            dma((lists, chunks, chips)),
            dma((lists, chunks, chips)),
            dma((lists, chunks, chips)),
            dma((lists, chunks, chips)),
        ],
        compiler_params=pltpu.CompilerParams(
            collective_id=1 + index, has_side_effects=True, vmem_limit_bytes=62 * 1024 * 1024
        ),
        name="work" + str(rows),
    )(near, slots, ao_tiles, packed, coeffs)


CLASSES = (6, 7, 8, 9, 10)


def local(ao_tiles, mo_coeffs, mu_blocks, nu_blocks, tile_live, batch_target, batch_count):
    tiles, _, nu_width, _ = ao_tiles.shape
    tasks, occs = lax.axis_size("task"), lax.axis_size("occ")
    nu_range = mo_coeffs.shape[0] // nu_width
    step = GROUP // occs
    rows = up(-(-tiles // occs), step)
    classes = [c * step for c in CLASSES if c * step < rows] + [rows]
    coeff = mo_coeffs.T

    meta, slots = make_plan(nu_range, tile_live, batch_target, batch_count, mu_blocks, nu_blocks)
    near, coeffs, packed, picked = exchange(
        tasks, occs, rows, classes, slots, meta.reshape(-1, LANES), coeff, ao_tiles
    )
    branches = [partial(work, tasks, occs, nu_range, index, size, step) for index, size in enumerate(classes)]
    turned = lax.switch(picked[0], branches, near.reshape(-1), slots, ao_tiles, packed, coeffs)
    return jnp.swapaxes(turned, 0, 1)


def solution(mesh):
    in_specs = (
        P("task", None, None, None),
        P(None, "occ"),
        P("task"),
        P("task"),
        P("task"),
        P("task"),
        P("task"),
    )
    out_specs = P("occ", None, "task")
    return jax.shard_map(local, mesh=mesh, in_specs=in_specs, out_specs=out_specs, check_vma=False)
```

```python
from functools import partial

import jax
import jax.numpy as jnp
import numpy as np
from jax import lax
from jax.experimental import pallas as pl
from jax.experimental.pallas import tpu as pltpu
from jax.sharding import PartitionSpec as P

SPREAD = 3
GROUP = 8
LANES = 128
F32 = jnp.float32
BF16 = jnp.bfloat16
MESH = pl.DeviceIdType.MESH


def up(value, unit):
    return -(-value // unit) * unit


def list_room(tiles):
    return up(tiles + 1, LANES)


def meta_rows(tiles):
    return up(SPREAD * list_room(tiles) // LANES + 1, 8)


def plan_kernel(nu_range, live, target, count, mu, nu, meta_ref, slots_ref, live_ref, target_ref, count_ref, mu_ref, nu_ref, landed):
    sources = (live, target, count, mu, nu)
    held = (live_ref, target_ref, count_ref, mu_ref, nu_ref)
    copies = [pltpu.make_async_copy(src, dst, landed.at[k]) for k, (src, dst) in enumerate(zip(sources, held))]
    for copy in copies:
        copy.start()
    tiles = live_ref.shape[0]
    per_batch = tiles // target_ref.shape[0]
    room = list_room(tiles)
    counts_at = SPREAD * room
    unrolled = 8

    def clear(k, carry):
        for b in range(unrolled):
            meta_ref[counts_at + k * unrolled + b] = 0
        return carry

    def clear_lists(k, carry):
        for s in range(SPREAD):
            for b in range(unrolled):
                meta_ref[s * room + k * unrolled + b] = 0
                slots_ref[s * room + k * unrolled + b] = 0
        return carry

    lax.fori_loop(0, LANES // unrolled, clear, 0)
    lax.fori_loop(0, min(up(tiles, 2 * GROUP) + 4 * GROUP, room) // unrolled, clear_lists, 0)
    for copy in copies:
        copy.wait()

    def take_batch(batch, carry):
        target = target_ref[batch]
        at = meta_ref[counts_at + target]
        for q in range(per_batch):
            tile = batch * per_batch + q
            slots_ref[target * room + at] = tile
            meta_ref[target * room + at] = mu_ref[tile] * nu_range + nu_ref[tile]
            at = at + live_ref[tile]
        meta_ref[counts_at + target] = at
        return carry

    lax.fori_loop(0, count_ref[0], take_batch, 0)


def make_plan(nu_range, tile_live, batch_target, batch_count, mu_blocks, nu_blocks):
    smem = pl.BlockSpec(memory_space=pltpu.SMEM)
    tiles = tile_live.shape[0]
    ins = (tile_live, batch_target, batch_count, mu_blocks, nu_blocks)
    return pl.pallas_call(
        partial(plan_kernel, nu_range),
        out_shape=(
            jax.ShapeDtypeStruct((meta_rows(tiles) * LANES,), jnp.int32),
            jax.ShapeDtypeStruct((SPREAD * list_room(tiles),), jnp.int32),
        ),
        in_specs=[pl.BlockSpec(memory_space=pl.ANY)] * len(ins),
        out_specs=(smem, smem),
        scratch_shapes=[pltpu.SMEM(x.shape, jnp.int32) for x in ins] + [pltpu.SemaphoreType.DMA((len(ins),))],
        name="plan",
    )(*ins)


class Place:
    def __init__(self, tasks, occs):
        self.tasks, self.occs, self.chips = tasks, occs, occs // 2
        self.task, self.me = lax.axis_index("task"), lax.axis_index("occ")
        self.chip, self.core = self.me // 2, self.me % 2

    def ahead(self, hops):
        return {"task": (self.task + hops) % self.tasks, "occ": self.me}

    def across_index(self, hops):
        return (self.chip + hops + self.chips) % self.chips * 2 + self.core

    def across(self, hops):
        return {"task": self.task, "occ": self.across_index(hops)}

    def sibling_index(self):
        return self.chip * 2 + 1 - self.core

    def sibling(self):
        return {"task": self.task, "occ": self.sibling_index()}

    def greet(self, hops, inside=True):
        barrier = pltpu.get_barrier_semaphore()
        others = [self.ahead(h) for h in hops]
        if inside:
            others += [self.across(h) for h in range(1, self.chips)] + [self.sibling()]
        for other in others:
            pl.semaphore_signal(barrier, inc=1, device_id=other, device_id_type=MESH)
        pl.semaphore_wait(barrier, len(others))


def send(src, dst, sems, device):
    return pltpu.make_async_remote_copy(
        src_ref=src, dst_ref=dst, send_sem=sems[0], recv_sem=sems[1], device_id=device, device_id_type=MESH
    )


def own_steps_of(chunks):
    return (chunks + 1) // 2


def exchange_kernel(
    tasks, occs, counts_row, limits, slots_ref, meta, coeff, tiles, near, coeffs, packed, picked, *refs
):
    far, held, shares, told, heard, over, overed, side, sided, kept, taken, put = refs
    place = Place(tasks, occs)
    count = tiles.shape[0]
    parts, rows = taken.shape[0], packed.shape[1]
    part, band = count // parts, rows // put.shape[0]
    takes = [
        pltpu.make_async_copy(tiles.at[pl.ds(k * part, part)], held.at[pl.ds(k * part, part)], taken.at[k])
        for k in range(parts)
    ]
    for take in takes:
        take.start()
    mine = pltpu.make_async_copy(meta, near.at[0], kept.at[0])
    mine.start()
    own = pltpu.make_async_copy(coeff, coeffs.at[place.me], kept.at[1])
    own.start()
    place.greet(range(1, tasks))

    def tell(hops):
        dst = near.at[hops] if hops < SPREAD else far.at[hops - SPREAD]
        return send(meta, dst, (told.at[hops - 1], heard.at[hops - 1]), place.ahead(hops))

    def cross(hops):
        return send(coeff, coeffs.at[place.me], (over.at[hops - 1], overed.at[hops - 1]), place.across(hops))

    def aside(hops):
        owner = place.across_index(-hops)
        src = coeffs.at[owner] if hops else coeff
        return send(src, coeffs.at[owner], (side.at[hops], sided.at[hops]), place.sibling())

    for hops in range(1, place.chips):
        cross(hops).start()
    for hops in range(1, tasks):
        tell(hops).start()
    aside(0).start()
    for take in takes:
        take.wait()
    room = list_room(count)

    def store(k):
        at = pl.ds(k * band, band)
        return pltpu.make_async_copy(shares.at[:, at], packed.at[:, at], put.at[k])

    def pack(k, carry):
        for d in range(band):
            row = k * band + d
            for s in range(1, SPREAD):
                shares[s - 1, row] = held[slots_ref[s * room + row * occs + place.me]]

        @pl.when(k >= 1)
        def _():
            store(k - 1).start()

        return carry

    bands = put.shape[0]
    lax.fori_loop(0, bands, pack, 0)
    store(bands - 1).start()
    for hops in range(1, place.chips):
        cross(hops).wait_recv()
        aside(hops).start()
    mine.wait()
    own.wait()
    for hops in range(1, tasks):
        tell(hops).wait()
    most = jnp.zeros((1, LANES), jnp.int32)
    for ref, filled in ((near, SPREAD), (far, tasks - SPREAD)):
        for k in range(filled):
            most = jnp.maximum(most, ref[k, counts_row : counts_row + 1, :])
    lane = lax.broadcasted_iota(jnp.int32, (1, LANES), 1)
    own_most = jnp.max(jnp.where(lane == 0, most, 0))
    moved = jnp.max(jnp.where((lane >= 1) & (lane < SPREAD), most, 0))
    index = jnp.int32(0)
    for moves, owns in limits[:-1]:
        index = index + jnp.where((moved > moves) | (own_most > owns), 1, 0)
    picked[0] = index

    def stored(k, carry):
        store(k).wait()
        return carry

    lax.fori_loop(0, bands, stored, 0)
    for hops in range(1, place.chips):
        cross(hops).wait_send()
    for hops in range(place.chips):
        aside(hops).wait()


def exchange(tasks, occs, rows, limits, slots, meta, coeff, ao_tiles):
    anywhere = pl.BlockSpec(memory_space=pltpu.HBM)
    smem = pl.BlockSpec(memory_space=pltpu.SMEM)
    tiles = ao_tiles.shape[0]
    chips = occs // 2
    dma = pltpu.SemaphoreType.DMA
    shares = (SPREAD - 1, rows) + ao_tiles.shape[1:]
    return pl.pallas_call(
        partial(exchange_kernel, tasks, occs, SPREAD * list_room(tiles) // LANES, limits),
        out_shape=(
            jax.ShapeDtypeStruct((SPREAD,) + meta.shape, meta.dtype),
            jax.ShapeDtypeStruct((occs,) + coeff.shape, coeff.dtype),
            jax.ShapeDtypeStruct(shares, ao_tiles.dtype),
            jax.ShapeDtypeStruct((1,), jnp.int32),
        ),
        in_specs=[smem, anywhere, anywhere, anywhere],
        out_specs=(pl.BlockSpec(memory_space=pltpu.VMEM), anywhere, anywhere, smem),
        scratch_shapes=[
            pltpu.VMEM((tasks - SPREAD,) + meta.shape, meta.dtype),
            pltpu.VMEM(ao_tiles.shape, ao_tiles.dtype),
            pltpu.VMEM(shares, ao_tiles.dtype),
            dma((tasks - 1,)),
            dma((tasks - 1,)),
            dma((chips,)),
            dma((chips,)),
            dma((chips,)),
            dma((chips,)),
            dma((2,)),
            dma((8 if tiles % 8 == 0 else 1,)),
            dma((5 if rows % 5 == 0 else 1,)),
        ],
        compiler_params=pltpu.CompilerParams(
            collective_id=0, has_side_effects=True, vmem_limit_bytes=48 * 1024 * 1024
        ),
        name="exchange",
    )(slots, meta, coeff, ao_tiles)


def work_kernel(tasks, occs, nu_range, chunks, step, ratio, near_ref, slots_ref, tiles, packed, coeffs, total, *refs):
    recv, held, flat, spread_rows, coeff_i, left_a, left_b, lhs_a, lhs_b, stage, mixed, mu_rows = refs[:12]
    taken, on, oned, over, overed, side, sided = refs[12:]
    place = Place(tasks, occs)
    count, mu_width, nu_width, kl = tiles.shape
    all_occ, tall = total.shape[:2]
    occ = coeffs.shape[1]
    room = list_room(count)
    meta = near_ref.shape[0] // SPREAD
    counts_at = SPREAD * room
    per = LANES // nu_width
    lists = range(SPREAD - 1)
    hopses = range(1, place.chips)
    own_steps = own_steps_of(chunks)
    ticks, size = chunks * ratio, step // ratio

    parts = taken.shape[0]
    part = count // parts
    takes = [
        pltpu.make_async_copy(tiles.at[pl.ds(k * part, part)], held.at[pl.ds(k * part, part)], taken.at[k])
        for k in range(parts)
    ]

    def onward(s, k):
        return send(
            packed.at[s, pl.ds(k * size, size)],
            recv.at[s, place.me, pl.ds(k * size, size)],
            (on.at[s, k], oned.at[s, k]),
            place.ahead(s + 1),
        )

    def cross(s, k, hops):
        block = recv.at[s, place.me, pl.ds(k * size, size)]
        return send(block, block, (over.at[s, k, hops - 1], overed.at[s, k, hops - 1]), place.across(hops))

    def aside(s, k, hops):
        block = recv.at[s, place.across_index(-hops), pl.ds(k * size, size)]
        return send(block, block, (side.at[s, k, hops], sided.at[s, k, hops]), place.sibling())

    def loop(upper, act):
        def body(k, carry):
            act(k)
            return carry

        lax.fori_loop(0, upper, body, 0)

    def clear(ref, pieces):
        size = ref.shape[0] // pieces

        def body(k):
            ref[pl.ds(k * size, size)] = jnp.zeros((size,) + ref.shape[1:], ref.dtype)

        loop(pieces, body)

    def launch(k):
        for s in lists:
            onward(s, k).start()

    def spread(k):
        for s in lists:
            onward(s, k).wait_recv()
            for hops in hopses:
                cross(s, k, hops).start()
            aside(s, k, 0).start()

    def relay(k):
        for s in lists:
            for hops in hopses:
                cross(s, k, hops).wait_recv()
                aside(s, k, hops).start()

    for take in takes:
        take.start()
    clear(left_a.at[0], 16)
    clear(left_a.at[1], 16)
    place.greet((1, 2, tasks - 1, tasks - 2))
    loop(ticks, launch)
    clear(left_b.at[0], 16)
    clear(left_b.at[1], 16)
    clear(total, 20)
    turn = (((0,), (0,)), ((), ()))
    unit = (
        lax.broadcasted_iota(jnp.int32, (tall, occ), 0) == lax.broadcasted_iota(jnp.int32, (tall, occ), 1)
    ).astype(F32).astype(BF16)
    rows_i = lax.dot_general(coeffs[place.me], unit[:occ], turn, preferred_element_type=F32)
    coeff_i[...] = rows_i.reshape(coeff_i.shape)
    for q in range(occs):
        flat[q * occ : (q + 1) * occ, :] = coeffs[q].astype(F32)
    source = lax.broadcasted_iota(jnp.int32, (LANES, per * LANES), 0)
    column = lax.broadcasted_iota(jnp.int32, (LANES, per * LANES), 1)
    repeat = (source == column // LANES * nu_width + column % nu_width).astype(F32).astype(BF16)

    def lay(c, carry):
        block = flat[:, pl.ds(pl.multiple_of(c * LANES, LANES), LANES)].astype(BF16)
        got = jnp.dot(block, repeat, preferred_element_type=F32)
        for r in range(per):
            spread_rows[c * per + r] = got[:, r * LANES : (r + 1) * LANES]
        return carry

    lax.fori_loop(0, flat.shape[1] // LANES, lay, 0)

    lane = lax.broadcasted_iota(jnp.int32, (1, LANES), 1) // nu_width
    band = all_occ // 4
    width = mu_width * GROUP
    steps = own_steps + chunks
    lead = min(own_steps, 2 * ratio)
    far_off = steps + own_steps + 1

    def counted(s):
        return near_ref[s * meta + counts_at + s]

    def list_of(e, g):
        j = (e + far_off - own_steps) // far_off
        own, c = e * 2 * GROUP + g * GROUP, (e - own_steps) * GROUP
        base = (1 - j) * own + j * ((g + 1) * (meta + room) + c)
        return base, (1 - j) * (counted(0) - own) + j * (counted(g + 1) - c)

    def build(e, g, left, lhs):
        base, valid = list_of(e, g)
        for b in range(GROUP):
            live = jnp.where(b < valid, 1.0, 0.0)
            mask = jnp.where(lane == b % per, live, 0.0)
            nu = lax.rem(near_ref[base + b], nu_range)
            left[b // per, pl.ds(b, all_occ, stride=GROUP), :] = spread_rows[nu] * mask
        for h in range(GROUP // per):
            lhs[:, h * LANES : (h + 1) * LANES] = left[h].astype(BF16)

    def first(g, lhs):
        for p in range(mu_width // 2):
            halves = [stage[g * GROUP : (g + 1) * GROUP, m].reshape(GROUP * nu_width, kl) for m in (2 * p, 2 * p + 1)]
            rhs = jnp.concatenate(halves, axis=1)
            at = g * width + 2 * p * GROUP
            for r in range(4):
                got = jnp.dot(
                    lhs[r * band * GROUP : (r + 1) * band * GROUP, :], rhs, preferred_element_type=F32
                ).reshape(band, GROUP, 2 * kl)
                got = jnp.concatenate([got[:, :, :kl], got[:, :, kl:]], axis=1)
                mixed[r * band : (r + 1) * band, at : at + 2 * GROUP, :] = got.astype(BF16)

    def second(e):
        for g in range(2):
            base = list_of(e, g)[0]
            for b in range(GROUP):
                mu = lax.div(near_ref[base + b], nu_range)
                mu_rows[pl.ds(g * width + b, mu_width, stride=GROUP), :] = coeff_i[mu]
        left_i = lax.dot_general(
            unit, mu_rows[...].astype(BF16), (((1,), (1,)), ((), ())), preferred_element_type=F32
        ).astype(BF16)
        for j in range(0, all_occ, 2):
            both = jnp.concatenate([mixed[j], mixed[j + 1]], axis=1)
            got = jnp.dot(left_i, both, preferred_element_type=F32)
            total[j] += got[:, :kl]
            total[j + 1] += got[:, kl:]

    build(0, 0, left_a, lhs_a)
    for take in takes:
        take.wait()

    def within(tick, act):
        @pl.when(tick >= 0)
        def _():
            @pl.when(tick < ticks)
            def _():
                act(tick)

    def take_step(e):
        c = e - own_steps

        @pl.when(c < 0)
        def _():
            @pl.when(e == 1)
            def _():
                spread(0)

            @pl.when(c == -1)
            def _():
                spread(1)
                relay(0)

            for b in range(2 * GROUP):
                stage[b] = held[slots_ref[e * 2 * GROUP + b]]

        @pl.when(c >= 0)
        def _():
            within(lead + c, spread)
            for s in lists:
                for d in range(ratio):
                    for hops in range(place.chips):
                        aside(s, c * ratio + d, hops).wait_recv()
                for b in range(GROUP):
                    stage[s * GROUP + b] = recv[s, b % occs, c * step + b // occs]

        build(e, 1, left_b, lhs_b)
        first(0, lhs_a)
        first(1, lhs_b)

        @pl.when(c < 0)
        def _():
            pass

        @pl.when(c >= 0)
        def _():
            pass

        build(e + 1, 0, left_a, lhs_a)
        second(e)

        @pl.when(c >= 0)
        def _():
            within(lead + c - 1, relay)

    loop(steps, take_step)

    def finish(k):
        for s in lists:
            onward(s, k).wait_send()
            for hops in hopses:
                cross(s, k, hops).wait_send()
            for hops in range(place.chips):
                aside(s, k, hops).wait_send()

    loop(ticks, finish)


def work(tasks, occs, nu_range, index, rows, step, near, slots, ao_tiles, packed, coeffs):
    anywhere = pl.BlockSpec(memory_space=pl.ANY)
    smem = pl.BlockSpec(memory_space=pltpu.SMEM)
    vmem = pltpu.VMEM
    chips = occs // 2
    chunks = rows // step
    ratio = 1
    ticks = chunks * ratio
    dma = pltpu.SemaphoreType.DMA
    lists = SPREAD - 1
    count, mu_width, nu_width, kl = ao_tiles.shape
    _, occ, basis = coeffs.shape
    all_occ, tall = occs * occ, up(occ, 8)
    depth = 2 * GROUP * mu_width
    return pl.pallas_call(
        partial(work_kernel, tasks, occs, nu_range, chunks, step, ratio),
        out_shape=jax.ShapeDtypeStruct((all_occ, tall, kl), F32),
        in_specs=[smem, smem, anywhere, anywhere, pl.BlockSpec(memory_space=pltpu.VMEM)],
        out_specs=pl.BlockSpec(memory_space=pltpu.VMEM),
        scratch_shapes=[
            vmem((lists, occs, rows) + ao_tiles.shape[1:], BF16),
            vmem(ao_tiles.shape, BF16),
            vmem((all_occ, basis), F32),
            vmem((nu_range, all_occ, LANES), F32),
            vmem((basis // mu_width, mu_width, occ), F32),
            vmem((GROUP * nu_width // LANES, all_occ * GROUP, LANES), F32),
            vmem((GROUP * nu_width // LANES, all_occ * GROUP, LANES), F32),
            vmem((all_occ * GROUP, GROUP * nu_width), BF16),
            vmem((all_occ * GROUP, GROUP * nu_width), BF16),
            vmem((2 * GROUP,) + ao_tiles.shape[1:], BF16),
            vmem((all_occ, depth, kl), BF16),
            vmem((depth, occ), F32),
            dma((8 if count % 8 == 0 else 1,)),
            dma((lists, ticks)),
            dma((lists, ticks)),
            dma((lists, ticks, chips)),
            dma((lists, ticks, chips)),
            dma((lists, ticks, chips)),
            dma((lists, ticks, chips)),
        ],
        compiler_params=pltpu.CompilerParams(
            collective_id=1 + index, has_side_effects=True, vmem_limit_bytes=66 * 1000 * 1000
        ),
        name="work" + str(rows),
    )(near, slots, ao_tiles, packed, coeffs)


def turn_kernel(turned, out, held, made, taken, put):
    parts, _, rows, kl = held.shape
    kept = out.shape[0]
    takes = [
        pltpu.make_async_copy(turned.at[:, pl.ds(p * rows, rows)], held.at[p], taken.at[p]) for p in range(parts)
    ]
    for take in takes:
        take.start()
    puts = []
    for p in range(parts):
        takes[p].wait()
        have = min(rows, kept - p * rows)
        block = held[p]
        for i in range(have):
            made[p * rows + i] = block[:, i, :]
        puts.append(
            pltpu.make_async_copy(made.at[pl.ds(p * rows, have)], out.at[pl.ds(p * rows, have)], put.at[p])
        )
        puts[-1].start()
    for copy in puts:
        copy.wait()


def turn_back(turned, occ):
    all_occ, tall, kl = turned.shape
    parts = tall // 8
    anywhere = pl.BlockSpec(memory_space=pl.ANY)
    return pl.pallas_call(
        turn_kernel,
        out_shape=jax.ShapeDtypeStruct((occ, all_occ, kl), F32),
        in_specs=[anywhere],
        out_specs=anywhere,
        scratch_shapes=[
            pltpu.VMEM((parts, all_occ, 8, kl), F32),
            pltpu.VMEM((occ, all_occ, kl), F32),
            pltpu.SemaphoreType.DMA((parts,)),
            pltpu.SemaphoreType.DMA((parts,)),
        ],
        compiler_params=pltpu.CompilerParams(vmem_limit_bytes=48 * 1024 * 1024),
        name="turn",
    )(turned)


CLASSES = (6, 7, 8, 9, 10)


def local(ao_tiles, mo_coeffs, mu_blocks, nu_blocks, tile_live, batch_target, batch_count):
    tiles, _, nu_width, _ = ao_tiles.shape
    tasks, occs = lax.axis_size("task"), lax.axis_size("occ")
    nu_range = mo_coeffs.shape[0] // nu_width
    step = GROUP // occs
    rows = up(-(-tiles // occs), step)
    classes = [c * step for c in CLASSES if c * step < rows] + [rows]
    limits = [(r * occs, 2 * GROUP * own_steps_of(r // step)) for r in classes]
    coeff = mo_coeffs.T

    meta, slots = make_plan(nu_range, tile_live, batch_target, batch_count, mu_blocks, nu_blocks)
    near, coeffs, packed, picked = exchange(
        tasks, occs, rows, limits, slots, meta.reshape(-1, LANES), coeff, ao_tiles
    )
    branches = [partial(work, tasks, occs, nu_range, index, size, step) for index, size in enumerate(classes)]
    turned = lax.switch(picked[0], branches, near.reshape(-1), slots, ao_tiles, packed, coeffs)
    return turn_back(turned, coeff.shape[0])


def solution(mesh):
    in_specs = (
        P("task", None, None, None),
        P(None, "occ"),
        P("task"),
        P("task"),
        P("task"),
        P("task"),
        P("task"),
    )
    out_specs = P("occ", None, "task")
    return jax.shard_map(local, mesh=mesh, in_specs=in_specs, out_specs=out_specs, check_vma=False)
```

```python
from functools import partial

import jax
import jax.numpy as jnp
import numpy as np
from jax import lax
from jax.experimental import pallas as pl
from jax.experimental.pallas import tpu as pltpu
from jax.sharding import PartitionSpec as P

SPREAD = 3
GROUP = 8
LANES = 128
F32 = jnp.float32
BF16 = jnp.bfloat16
MESH = pl.DeviceIdType.MESH


def up(value, unit):
    return -(-value // unit) * unit


def list_room(tiles):
    return up(tiles + 1, LANES)


def meta_rows(tiles):
    return up(SPREAD * list_room(tiles) // LANES + 1, 8)


def plan_kernel(nu_range, live, target, count, mu, nu, meta_ref, slots_ref, live_ref, target_ref, count_ref, mu_ref, nu_ref, landed):
    sources = (live, target, count, mu, nu)
    held = (live_ref, target_ref, count_ref, mu_ref, nu_ref)
    copies = [pltpu.make_async_copy(src, dst, landed.at[k]) for k, (src, dst) in enumerate(zip(sources, held))]
    for copy in copies:
        copy.start()
    tiles = live_ref.shape[0]
    per_batch = tiles // target_ref.shape[0]
    room = list_room(tiles)
    counts_at = SPREAD * room
    unrolled = 8

    def clear(k, carry):
        for b in range(unrolled):
            meta_ref[counts_at + k * unrolled + b] = 0
        return carry

    def clear_lists(k, carry):
        for s in range(SPREAD):
            for b in range(unrolled):
                meta_ref[s * room + k * unrolled + b] = 0
                slots_ref[s * room + k * unrolled + b] = 0
        return carry

    lax.fori_loop(0, LANES // unrolled, clear, 0)
    lax.fori_loop(0, min(up(tiles, 2 * GROUP) + 4 * GROUP, room) // unrolled, clear_lists, 0)
    for copy in copies:
        copy.wait()

    def take_batch(batch, carry):
        target = target_ref[batch]
        at = meta_ref[counts_at + target]
        for q in range(per_batch):
            tile = batch * per_batch + q
            slots_ref[target * room + at] = tile
            meta_ref[target * room + at] = mu_ref[tile] * nu_range + nu_ref[tile]
            at = at + live_ref[tile]
        meta_ref[counts_at + target] = at
        return carry

    lax.fori_loop(0, count_ref[0], take_batch, 0)


def make_plan(nu_range, tile_live, batch_target, batch_count, mu_blocks, nu_blocks):
    smem = pl.BlockSpec(memory_space=pltpu.SMEM)
    tiles = tile_live.shape[0]
    ins = (tile_live, batch_target, batch_count, mu_blocks, nu_blocks)
    return pl.pallas_call(
        partial(plan_kernel, nu_range),
        out_shape=(
            jax.ShapeDtypeStruct((meta_rows(tiles) * LANES,), jnp.int32),
            jax.ShapeDtypeStruct((SPREAD * list_room(tiles),), jnp.int32),
        ),
        in_specs=[pl.BlockSpec(memory_space=pl.ANY)] * len(ins),
        out_specs=(smem, smem),
        scratch_shapes=[pltpu.SMEM(x.shape, jnp.int32) for x in ins] + [pltpu.SemaphoreType.DMA((len(ins),))],
        name="plan",
    )(*ins)


class Place:
    def __init__(self, tasks, occs):
        self.tasks, self.occs, self.chips = tasks, occs, occs // 2
        self.task, self.me = lax.axis_index("task"), lax.axis_index("occ")
        self.chip, self.core = self.me // 2, self.me % 2

    def ahead(self, hops):
        return {"task": (self.task + hops) % self.tasks, "occ": self.me}

    def across_index(self, hops):
        return (self.chip + hops + self.chips) % self.chips * 2 + self.core

    def across(self, hops):
        return {"task": self.task, "occ": self.across_index(hops)}

    def sibling_index(self):
        return self.chip * 2 + 1 - self.core

    def sibling(self):
        return {"task": self.task, "occ": self.sibling_index()}

    def greet(self, hops, inside=True):
        barrier = pltpu.get_barrier_semaphore()
        others = [self.ahead(h) for h in hops]
        if inside:
            others += [self.across(h) for h in range(1, self.chips)] + [self.sibling()]
        for other in others:
            pl.semaphore_signal(barrier, inc=1, device_id=other, device_id_type=MESH)
        pl.semaphore_wait(barrier, len(others))


def send(src, dst, sems, device):
    return pltpu.make_async_remote_copy(
        src_ref=src, dst_ref=dst, send_sem=sems[0], recv_sem=sems[1], device_id=device, device_id_type=MESH
    )


def own_steps_of(chunks):
    return (chunks + 1) // 2


def exchange_kernel(
    tasks, occs, counts_row, limits, slots_ref, meta, coeff, tiles, near, coeffs, packed, early, picked, *refs
):
    far, held, shares, told, heard, over, overed, side, sided, on, oned, kept, taken, put = refs
    place = Place(tasks, occs)
    count = tiles.shape[0]
    parts, rows = taken.shape[0], packed.shape[1]
    part, band = count // parts, rows // put.shape[0]
    takes = [
        pltpu.make_async_copy(tiles.at[pl.ds(k * part, part)], held.at[pl.ds(k * part, part)], taken.at[k])
        for k in range(parts)
    ]
    for take in takes:
        take.start()
    mine = pltpu.make_async_copy(meta, near.at[0], kept.at[0])
    mine.start()
    own = pltpu.make_async_copy(coeff, coeffs.at[place.me], kept.at[1])
    own.start()
    place.greet(range(1, tasks))

    def tell(hops):
        dst = near.at[hops] if hops < SPREAD else far.at[hops - SPREAD]
        return send(meta, dst, (told.at[hops - 1], heard.at[hops - 1]), place.ahead(hops))

    def cross(hops):
        return send(coeff, coeffs.at[place.me], (over.at[hops - 1], overed.at[hops - 1]), place.across(hops))

    def aside(hops):
        owner = place.across_index(-hops)
        src = coeffs.at[owner] if hops else coeff
        return send(src, coeffs.at[owner], (side.at[hops], sided.at[hops]), place.sibling())

    def onward(s):
        share = shares.at[s, pl.ds(0, early.shape[1])]
        return send(share, early.at[s], (on.at[s], oned.at[s]), place.ahead(s + 1))

    for hops in range(1, place.chips):
        cross(hops).start()
    for hops in range(1, tasks):
        tell(hops).start()
    aside(0).start()
    for take in takes:
        take.wait()
    room = list_room(count)

    def store(k):
        at = pl.ds(k * band, band)
        return pltpu.make_async_copy(shares.at[:, at], packed.at[:, at], put.at[k])

    def pack(k, carry):
        for d in range(band):
            row = k * band + d
            for s in range(1, SPREAD):
                shares[s - 1, row] = held[slots_ref[s * room + row * occs + place.me]]

        @pl.when(k == 1)
        def _():
            for s in range(SPREAD - 1):
                onward(s).start()

        @pl.when(k >= 1)
        def _():
            store(k - 1).start()

        return carry

    bands = put.shape[0]
    lax.fori_loop(0, bands, pack, 0)
    store(bands - 1).start()
    for hops in range(1, place.chips):
        cross(hops).wait_recv()
        aside(hops).start()
    mine.wait()
    own.wait()
    for hops in range(1, tasks):
        tell(hops).wait()
    most = jnp.zeros((1, LANES), jnp.int32)
    for ref, filled in ((near, SPREAD), (far, tasks - SPREAD)):
        for k in range(filled):
            most = jnp.maximum(most, ref[k, counts_row : counts_row + 1, :])
    lane = lax.broadcasted_iota(jnp.int32, (1, LANES), 1)
    own_most = jnp.max(jnp.where(lane == 0, most, 0))
    moved = jnp.max(jnp.where((lane >= 1) & (lane < SPREAD), most, 0))
    index = jnp.int32(0)
    for moves, owns in limits[:-1]:
        index = index + jnp.where((moved > moves) | (own_most > owns), 1, 0)
    picked[0] = index

    def stored(k, carry):
        store(k).wait()
        return carry

    lax.fori_loop(0, bands, stored, 0)
    for s in range(SPREAD - 1):
        onward(s).wait()
    for hops in range(1, place.chips):
        cross(hops).wait_send()
    for hops in range(place.chips):
        aside(hops).wait()


def exchange(tasks, occs, rows, step, limits, slots, meta, coeff, ao_tiles):
    anywhere = pl.BlockSpec(memory_space=pl.ANY)
    smem = pl.BlockSpec(memory_space=pltpu.SMEM)
    tiles = ao_tiles.shape[0]
    chips = occs // 2
    dma = pltpu.SemaphoreType.DMA
    shares = (SPREAD - 1, rows) + ao_tiles.shape[1:]
    return pl.pallas_call(
        partial(exchange_kernel, tasks, occs, SPREAD * list_room(tiles) // LANES, limits),
        out_shape=(
            jax.ShapeDtypeStruct((SPREAD,) + meta.shape, meta.dtype),
            jax.ShapeDtypeStruct((occs,) + coeff.shape, coeff.dtype),
            jax.ShapeDtypeStruct(shares, ao_tiles.dtype),
            jax.ShapeDtypeStruct((SPREAD - 1, step) + ao_tiles.shape[1:], ao_tiles.dtype),
            jax.ShapeDtypeStruct((1,), jnp.int32),
        ),
        in_specs=[smem, anywhere, anywhere, anywhere],
        out_specs=(pl.BlockSpec(memory_space=pltpu.VMEM), anywhere, anywhere, anywhere, smem),
        scratch_shapes=[
            pltpu.VMEM((tasks - SPREAD,) + meta.shape, meta.dtype),
            pltpu.VMEM(ao_tiles.shape, ao_tiles.dtype),
            pltpu.VMEM(shares, ao_tiles.dtype),
            dma((tasks - 1,)),
            dma((tasks - 1,)),
            dma((chips,)),
            dma((chips,)),
            dma((chips,)),
            dma((chips,)),
            dma((SPREAD - 1,)),
            dma((SPREAD - 1,)),
            dma((2,)),
            dma((8 if tiles % 8 == 0 else 1,)),
            dma((5 if rows % 5 == 0 else 2,)),
        ],
        compiler_params=pltpu.CompilerParams(
            collective_id=0, has_side_effects=True, vmem_limit_bytes=66 * 1000 * 1000
        ),
        name="exchange",
    )(slots, meta, coeff, ao_tiles)


def work_kernel(tasks, occs, nu_range, chunks, step, ratio, near_ref, slots_ref, tiles, packed, early, coeffs, total, *refs):
    recv, held, flat, spread_rows, coeff_i, left_a, left_b, lhs_a, lhs_b, stage, mixed, mu_rows = refs[:12]
    taken, kept, on, oned, over, overed, side, sided = refs[12:]
    place = Place(tasks, occs)
    count, mu_width, nu_width, kl = tiles.shape
    all_occ, tall = total.shape[:2]
    occ = coeffs.shape[1]
    room = list_room(count)
    meta = near_ref.shape[0] // SPREAD
    counts_at = SPREAD * room
    per = LANES // nu_width
    lists = range(SPREAD - 1)
    hopses = range(1, place.chips)
    own_steps = own_steps_of(chunks)
    ticks, size = chunks * ratio, step // ratio

    parts = taken.shape[0]
    part = count // parts
    takes = [
        pltpu.make_async_copy(tiles.at[pl.ds(k * part, part)], held.at[pl.ds(k * part, part)], taken.at[k])
        for k in range(parts)
    ]

    def onward(s, k):
        return send(
            packed.at[s, pl.ds(k * size, size)],
            recv.at[s, place.me, pl.ds(k * size, size)],
            (on.at[s, k], oned.at[s, k]),
            place.ahead(s + 1),
        )

    def cross(s, k, hops):
        block = recv.at[s, place.me, pl.ds(k * size, size)]
        return send(block, block, (over.at[s, k, hops - 1], overed.at[s, k, hops - 1]), place.across(hops))

    def aside(s, k, hops):
        block = recv.at[s, place.across_index(-hops), pl.ds(k * size, size)]
        return send(block, block, (side.at[s, k, hops], sided.at[s, k, hops]), place.sibling())

    def loop(upper, act):
        def body(k, carry):
            act(k)
            return carry

        lax.fori_loop(0, upper, body, 0)

    def clear(ref, pieces):
        size = ref.shape[0] // pieces

        def body(k):
            ref[pl.ds(k * size, size)] = jnp.zeros((size,) + ref.shape[1:], ref.dtype)

        loop(pieces, body)

    keeps = [pltpu.make_async_copy(early.at[s], recv.at[s, place.me, pl.ds(0, step)], kept.at[s]) for s in lists]

    def launch(k):
        for s in lists:
            onward(s, k).start()

    def spread(k, came=None):
        for s in lists:
            (came or (lambda s: onward(s, k).wait_recv()))(s)
            for hops in hopses:
                cross(s, k, hops).start()
            aside(s, k, 0).start()

    def relay(k):
        for s in lists:
            for hops in hopses:
                cross(s, k, hops).wait_recv()
                aside(s, k, hops).start()

    for copy in keeps + takes:
        copy.start()
    clear(left_a.at[0], 16)
    clear(left_a.at[1], 16)
    place.greet((1, 2, tasks - 1, tasks - 2))
    lax.fori_loop(ratio, ticks, lambda k, carry: (launch(k), carry)[1], 0)
    for copy in keeps:
        copy.wait()
    for k in range(ratio):
        spread(k, lambda s: None)
    clear(left_b.at[0], 16)
    clear(left_b.at[1], 16)
    clear(total, 20)
    turn = (((0,), (0,)), ((), ()))
    unit = (
        lax.broadcasted_iota(jnp.int32, (tall, occ), 0) == lax.broadcasted_iota(jnp.int32, (tall, occ), 1)
    ).astype(F32).astype(BF16)
    rows_i = lax.dot_general(coeffs[place.me], unit[:occ], turn, preferred_element_type=F32)
    coeff_i[...] = rows_i.reshape(coeff_i.shape)
    for q in range(occs):
        flat[q * occ : (q + 1) * occ, :] = coeffs[q].astype(F32)
    source = lax.broadcasted_iota(jnp.int32, (LANES, per * LANES), 0)
    column = lax.broadcasted_iota(jnp.int32, (LANES, per * LANES), 1)
    repeat = (source == column // LANES * nu_width + column % nu_width).astype(F32).astype(BF16)

    def lay(c, carry):
        block = flat[:, pl.ds(pl.multiple_of(c * LANES, LANES), LANES)].astype(BF16)
        got = jnp.dot(block, repeat, preferred_element_type=F32)
        for r in range(per):
            spread_rows[c * per + r] = got[:, r * LANES : (r + 1) * LANES]
        return carry

    lax.fori_loop(0, flat.shape[1] // LANES, lay, 0)

    lane = lax.broadcasted_iota(jnp.int32, (1, LANES), 1) // nu_width
    band = all_occ // 4
    width = mu_width * GROUP
    steps = own_steps + chunks
    far_off = steps + own_steps + 1

    def counted(s):
        return near_ref[s * meta + counts_at + s]

    def list_of(e, g):
        j = (e + far_off - own_steps) // far_off
        own, c = e * 2 * GROUP + g * GROUP, (e - own_steps) * GROUP
        base = (1 - j) * own + j * ((g + 1) * (meta + room) + c)
        return base, (1 - j) * (counted(0) - own) + j * (counted(g + 1) - c)

    def build(e, g, left, lhs):
        base, valid = list_of(e, g)
        for b in range(GROUP):
            live = jnp.where(b < valid, 1.0, 0.0)
            mask = jnp.where(lane == b % per, live, 0.0)
            nu = lax.rem(near_ref[base + b], nu_range)
            left[b // per, pl.ds(b, all_occ, stride=GROUP), :] = spread_rows[nu] * mask
        for h in range(GROUP // per):
            lhs[:, h * LANES : (h + 1) * LANES] = left[h].astype(BF16)

    def first(g, lhs):
        for p in range(mu_width // 2):
            halves = [stage[g * GROUP : (g + 1) * GROUP, m].reshape(GROUP * nu_width, kl) for m in (2 * p, 2 * p + 1)]
            rhs = jnp.concatenate(halves, axis=1)
            at = g * width + 2 * p * GROUP
            for r in range(4):
                got = jnp.dot(
                    lhs[r * band * GROUP : (r + 1) * band * GROUP, :], rhs, preferred_element_type=F32
                ).reshape(band, GROUP, 2 * kl)
                got = jnp.concatenate([got[:, :, :kl], got[:, :, kl:]], axis=1)
                mixed[r * band : (r + 1) * band, at : at + 2 * GROUP, :] = got.astype(BF16)

    def second(e):
        for g in range(2):
            base = list_of(e, g)[0]
            for b in range(GROUP):
                mu = lax.div(near_ref[base + b], nu_range)
                mu_rows[pl.ds(g * width + b, mu_width, stride=GROUP), :] = coeff_i[mu]
        left_i = lax.dot_general(
            unit, mu_rows[...].astype(BF16), (((1,), (1,)), ((), ())), preferred_element_type=F32
        ).astype(BF16)
        for j in range(0, all_occ, 2):
            both = jnp.concatenate([mixed[j], mixed[j + 1]], axis=1)
            got = jnp.dot(left_i, both, preferred_element_type=F32)
            total[j] += got[:, :kl]
            total[j + 1] += got[:, kl:]

    build(0, 0, left_a, lhs_a)
    for take in takes:
        take.wait()
    def within(tick, act, least=0):
        @pl.when(tick >= least)
        def _():
            @pl.when(tick < ticks)
            def _():
                act(tick)

    def take_step(e):
        c = e - own_steps

        @pl.when(c < 0)
        def _():
            @pl.when(e == 1)
            def _():
                spread(1)
                relay(0)

            @pl.when(c == -1)
            def _():
                spread(2)

            for b in range(2 * GROUP):
                stage[b] = held[slots_ref[e * 2 * GROUP + b]]

        @pl.when(c >= 0)
        def _():
            within(c + 2, spread, 3)
            for s in lists:
                for d in range(ratio):
                    for hops in range(place.chips):
                        aside(s, c * ratio + d, hops).wait_recv()
                for b in range(GROUP):
                    stage[s * GROUP + b] = recv[s, b % occs, c * step + b // occs]

        build(e, 1, left_b, lhs_b)
        first(0, lhs_a)
        first(1, lhs_b)

        build(e + 1, 0, left_a, lhs_a)
        second(e)

        @pl.when(c == -1)
        def _():
            relay(1)

        @pl.when(c == 0)
        def _():
            relay(2)

        @pl.when(c >= 2)
        def _():
            within(c + 1, relay)

    loop(steps, take_step)

    def finish(k):
        @pl.when(k >= ratio)
        def _():
            for s in lists:
                onward(s, k).wait_send()

        for s in lists:
            for hops in hopses:
                cross(s, k, hops).wait_send()
            for hops in range(place.chips):
                aside(s, k, hops).wait_send()

    loop(ticks, finish)


def work(tasks, occs, nu_range, index, rows, step, near, slots, ao_tiles, packed, early, coeffs):
    anywhere = pl.BlockSpec(memory_space=pl.ANY)
    smem = pl.BlockSpec(memory_space=pltpu.SMEM)
    vmem = pltpu.VMEM
    chips = occs // 2
    chunks = rows // step
    ratio = 1
    ticks = chunks * ratio
    dma = pltpu.SemaphoreType.DMA
    lists = SPREAD - 1
    count, mu_width, nu_width, kl = ao_tiles.shape
    _, occ, basis = coeffs.shape
    all_occ, tall = occs * occ, up(occ, 8)
    depth = 2 * GROUP * mu_width
    return pl.pallas_call(
        partial(work_kernel, tasks, occs, nu_range, chunks, step, ratio),
        out_shape=jax.ShapeDtypeStruct((all_occ, tall, kl), F32),
        in_specs=[smem, smem, anywhere, anywhere, anywhere, pl.BlockSpec(memory_space=pltpu.VMEM)],
        out_specs=pl.BlockSpec(memory_space=pltpu.VMEM),
        scratch_shapes=[
            vmem((lists, occs, rows) + ao_tiles.shape[1:], BF16),
            vmem(ao_tiles.shape, BF16),
            vmem((all_occ, basis), F32),
            vmem((nu_range, all_occ, LANES), F32),
            vmem((basis // mu_width, mu_width, occ), F32),
            vmem((GROUP * nu_width // LANES, all_occ * GROUP, LANES), F32),
            vmem((GROUP * nu_width // LANES, all_occ * GROUP, LANES), F32),
            vmem((all_occ * GROUP, GROUP * nu_width), BF16),
            vmem((all_occ * GROUP, GROUP * nu_width), BF16),
            vmem((2 * GROUP,) + ao_tiles.shape[1:], BF16),
            vmem((all_occ, depth, kl), BF16),
            vmem((depth, occ), F32),
            dma((8 if count % 8 == 0 else 1,)),
            dma((lists,)),
            dma((lists, ticks)),
            dma((lists, ticks)),
            dma((lists, ticks, chips)),
            dma((lists, ticks, chips)),
            dma((lists, ticks, chips)),
            dma((lists, ticks, chips)),
        ],
        compiler_params=pltpu.CompilerParams(
            collective_id=1 + index, has_side_effects=True, vmem_limit_bytes=66 * 1000 * 1000
        ),
        name="work" + str(rows),
    )(near, slots, ao_tiles, packed, early, coeffs)


def turn_kernel(turned, out, held, made, taken, put):
    parts, _, rows, kl = held.shape
    kept = out.shape[0]
    takes = [
        pltpu.make_async_copy(turned.at[:, pl.ds(p * rows, rows)], held.at[p], taken.at[p]) for p in range(parts)
    ]
    for take in takes:
        take.start()
    puts = []
    for p in range(parts):
        takes[p].wait()
        have = min(rows, kept - p * rows)
        block = held[p]
        for i in range(have):
            made[p * rows + i] = block[:, i, :]
        puts.append(
            pltpu.make_async_copy(made.at[pl.ds(p * rows, have)], out.at[pl.ds(p * rows, have)], put.at[p])
        )
        puts[-1].start()
    for copy in puts:
        copy.wait()


def turn_back(turned, occ):
    all_occ, tall, kl = turned.shape
    parts = tall // 8
    anywhere = pl.BlockSpec(memory_space=pl.ANY)
    return pl.pallas_call(
        turn_kernel,
        out_shape=jax.ShapeDtypeStruct((occ, all_occ, kl), F32),
        in_specs=[anywhere],
        out_specs=anywhere,
        scratch_shapes=[
            pltpu.VMEM((parts, all_occ, 8, kl), F32),
            pltpu.VMEM((occ, all_occ, kl), F32),
            pltpu.SemaphoreType.DMA((parts,)),
            pltpu.SemaphoreType.DMA((parts,)),
        ],
        compiler_params=pltpu.CompilerParams(vmem_limit_bytes=48 * 1024 * 1024),
        name="turn",
    )(turned)


CLASSES = (6, 7, 8, 9, 10)


def local(ao_tiles, mo_coeffs, mu_blocks, nu_blocks, tile_live, batch_target, batch_count):
    tiles, _, nu_width, _ = ao_tiles.shape
    tasks, occs = lax.axis_size("task"), lax.axis_size("occ")
    nu_range = mo_coeffs.shape[0] // nu_width
    step = GROUP // occs
    rows = up(-(-tiles // occs), step)
    classes = [c * step for c in CLASSES if c * step < rows] + [rows]
    limits = [(r * occs, 2 * GROUP * own_steps_of(r // step)) for r in classes]
    coeff = mo_coeffs.T

    meta, slots = make_plan(nu_range, tile_live, batch_target, batch_count, mu_blocks, nu_blocks)
    near, coeffs, packed, early, picked = exchange(
        tasks, occs, rows, step, limits, slots, meta.reshape(-1, LANES), coeff, ao_tiles
    )
    branches = [partial(work, tasks, occs, nu_range, index, size, step) for index, size in enumerate(classes)]
    turned = lax.switch(picked[0], branches, near.reshape(-1), slots, ao_tiles, packed, early, coeffs)
    return turn_back(turned, coeff.shape[0])


def solution(mesh):
    in_specs = (
        P("task", None, None, None),
        P(None, "occ"),
        P("task"),
        P("task"),
        P("task"),
        P("task"),
        P("task"),
    )
    out_specs = P("occ", None, "task")
    return jax.shard_map(local, mesh=mesh, in_specs=in_specs, out_specs=out_specs, check_vma=False)
```

```python
from functools import partial

import jax
import jax.numpy as jnp
import numpy as np
from jax import lax
from jax.experimental import pallas as pl
from jax.experimental.pallas import tpu as pltpu
from jax.sharding import PartitionSpec as P

SPREAD = 3
GROUP = 8
LANES = 128
F32 = jnp.float32
BF16 = jnp.bfloat16
MESH = pl.DeviceIdType.MESH


def up(value, unit):
    return -(-value // unit) * unit


def list_room(tiles):
    return up(tiles + 1, LANES)


def meta_rows(tiles):
    return up(SPREAD * list_room(tiles) // LANES + 1, 8)


def plan_kernel(nu_range, live, target, count, mu, nu, meta_ref, slots_ref, live_ref, target_ref, count_ref, mu_ref, nu_ref, landed):
    sources = (live, target, count, mu, nu)
    held = (live_ref, target_ref, count_ref, mu_ref, nu_ref)
    copies = [pltpu.make_async_copy(src, dst, landed.at[k]) for k, (src, dst) in enumerate(zip(sources, held))]
    for copy in copies:
        copy.start()
    tiles = live_ref.shape[0]
    per_batch = tiles // target_ref.shape[0]
    room = list_room(tiles)
    counts_at = SPREAD * room
    unrolled = 8

    def clear(k, carry):
        for b in range(unrolled):
            meta_ref[counts_at + k * unrolled + b] = 0
        return carry

    def clear_lists(k, carry):
        for s in range(SPREAD):
            for b in range(unrolled):
                meta_ref[s * room + k * unrolled + b] = 0
                slots_ref[s * room + k * unrolled + b] = 0
        return carry

    lax.fori_loop(0, LANES // unrolled, clear, 0)
    lax.fori_loop(0, min(up(tiles, 2 * GROUP) + 4 * GROUP, room) // unrolled, clear_lists, 0)
    for copy in copies:
        copy.wait()

    def take_batch(batch, carry):
        target = target_ref[batch]
        at = meta_ref[counts_at + target]
        for q in range(per_batch):
            tile = batch * per_batch + q
            slots_ref[target * room + at] = tile
            meta_ref[target * room + at] = mu_ref[tile] * nu_range + nu_ref[tile]
            at = at + live_ref[tile]
        meta_ref[counts_at + target] = at
        return carry

    lax.fori_loop(0, count_ref[0], take_batch, 0)


def make_plan(nu_range, tile_live, batch_target, batch_count, mu_blocks, nu_blocks):
    smem = pl.BlockSpec(memory_space=pltpu.SMEM)
    tiles = tile_live.shape[0]
    ins = (tile_live, batch_target, batch_count, mu_blocks, nu_blocks)
    return pl.pallas_call(
        partial(plan_kernel, nu_range),
        out_shape=(
            jax.ShapeDtypeStruct((meta_rows(tiles) * LANES,), jnp.int32),
            jax.ShapeDtypeStruct((SPREAD * list_room(tiles),), jnp.int32),
        ),
        in_specs=[pl.BlockSpec(memory_space=pl.ANY)] * len(ins),
        out_specs=(smem, smem),
        scratch_shapes=[pltpu.SMEM(x.shape, jnp.int32) for x in ins] + [pltpu.SemaphoreType.DMA((len(ins),))],
        name="plan",
    )(*ins)


class Place:
    def __init__(self, tasks, occs):
        self.tasks, self.occs, self.chips = tasks, occs, occs // 2
        self.task, self.me = lax.axis_index("task"), lax.axis_index("occ")
        self.chip, self.core = self.me // 2, self.me % 2

    def ahead(self, hops):
        return {"task": (self.task + hops) % self.tasks, "occ": self.me}

    def across_index(self, hops):
        return (self.chip + hops + self.chips) % self.chips * 2 + self.core

    def across(self, hops):
        return {"task": self.task, "occ": self.across_index(hops)}

    def sibling_index(self):
        return self.chip * 2 + 1 - self.core

    def sibling(self):
        return {"task": self.task, "occ": self.sibling_index()}

    def greet(self, hops, inside=True):
        barrier = pltpu.get_barrier_semaphore()
        others = [self.ahead(h) for h in hops]
        if inside:
            others += [self.across(h) for h in range(1, self.chips)] + [self.sibling()]
        for other in others:
            pl.semaphore_signal(barrier, inc=1, device_id=other, device_id_type=MESH)
        pl.semaphore_wait(barrier, len(others))


def send(src, dst, sems, device):
    return pltpu.make_async_remote_copy(
        src_ref=src, dst_ref=dst, send_sem=sems[0], recv_sem=sems[1], device_id=device, device_id_type=MESH
    )


def own_steps_of(chunks):
    return (chunks + 1) // 2


def exchange_kernel(
    tasks, occs, counts_row, limits, slots_ref, meta, coeff, tiles, near, coeffs, packed, early, picked, *refs
):
    far, held, shares, told, heard, over, overed, side, sided, on, oned, kept, taken, put = refs
    place = Place(tasks, occs)
    count = tiles.shape[0]
    parts, rows = taken.shape[0], packed.shape[1]
    part, band = count // parts, rows // put.shape[0]
    takes = [
        pltpu.make_async_copy(tiles.at[pl.ds(k * part, part)], held.at[pl.ds(k * part, part)], taken.at[k])
        for k in range(parts)
    ]
    for take in takes:
        take.start()
    mine = pltpu.make_async_copy(meta, near.at[0], kept.at[0])
    mine.start()
    own = pltpu.make_async_copy(coeff, coeffs.at[place.me], kept.at[1])
    own.start()
    place.greet(range(1, tasks))

    def tell(hops):
        dst = near.at[hops] if hops < SPREAD else far.at[hops - SPREAD]
        return send(meta, dst, (told.at[hops - 1], heard.at[hops - 1]), place.ahead(hops))

    def cross(hops):
        return send(coeff, coeffs.at[place.me], (over.at[hops - 1], overed.at[hops - 1]), place.across(hops))

    def aside(hops):
        owner = place.across_index(-hops)
        src = coeffs.at[owner] if hops else coeff
        return send(src, coeffs.at[owner], (side.at[hops], sided.at[hops]), place.sibling())

    def onward(s):
        share = shares.at[s, pl.ds(0, early.shape[1])]
        return send(share, early.at[s], (on.at[s], oned.at[s]), place.ahead(s + 1))

    for hops in range(1, place.chips):
        cross(hops).start()
    for hops in range(1, tasks):
        tell(hops).start()
    aside(0).start()
    for take in takes:
        take.wait()
    room = list_room(count)

    def store(k):
        at = pl.ds(k * band, band)
        return pltpu.make_async_copy(shares.at[:, at], packed.at[:, at], put.at[k])

    def pack(k, carry):
        for d in range(band):
            row = k * band + d
            for s in range(1, SPREAD):
                shares[s - 1, row] = held[slots_ref[s * room + row * occs + place.me]]

        @pl.when(k == 1)
        def _():
            for s in range(SPREAD - 1):
                onward(s).start()

        @pl.when(k >= 1)
        def _():
            store(k - 1).start()

        return carry

    bands = put.shape[0]
    lax.fori_loop(0, bands, pack, 0)
    store(bands - 1).start()
    for hops in range(1, place.chips):
        cross(hops).wait_recv()
        aside(hops).start()
    mine.wait()
    own.wait()
    for hops in range(1, tasks):
        tell(hops).wait()
    most = jnp.zeros((1, LANES), jnp.int32)
    for ref, filled in ((near, SPREAD), (far, tasks - SPREAD)):
        for k in range(filled):
            most = jnp.maximum(most, ref[k, counts_row : counts_row + 1, :])
    lane = lax.broadcasted_iota(jnp.int32, (1, LANES), 1)
    own_most = jnp.max(jnp.where(lane == 0, most, 0))
    moved = jnp.max(jnp.where((lane >= 1) & (lane < SPREAD), most, 0))
    index = jnp.int32(0)
    for moves, owns in limits[:-1]:
        index = index + jnp.where((moved > moves) | (own_most > owns), 1, 0)
    picked[0] = index

    def stored(k, carry):
        store(k).wait()
        return carry

    lax.fori_loop(0, bands, stored, 0)
    for s in range(SPREAD - 1):
        onward(s).wait()
    for hops in range(1, place.chips):
        cross(hops).wait_send()
    for hops in range(place.chips):
        aside(hops).wait()


def exchange(tasks, occs, rows, step, limits, slots, meta, coeff, ao_tiles):
    anywhere = pl.BlockSpec(memory_space=pl.ANY)
    smem = pl.BlockSpec(memory_space=pltpu.SMEM)
    tiles = ao_tiles.shape[0]
    chips = occs // 2
    dma = pltpu.SemaphoreType.DMA
    shares = (SPREAD - 1, rows) + ao_tiles.shape[1:]
    return pl.pallas_call(
        partial(exchange_kernel, tasks, occs, SPREAD * list_room(tiles) // LANES, limits),
        out_shape=(
            jax.ShapeDtypeStruct((SPREAD,) + meta.shape, meta.dtype),
            jax.ShapeDtypeStruct((occs,) + coeff.shape, coeff.dtype),
            jax.ShapeDtypeStruct(shares, ao_tiles.dtype),
            jax.ShapeDtypeStruct((SPREAD - 1, step) + ao_tiles.shape[1:], ao_tiles.dtype),
            jax.ShapeDtypeStruct((1,), jnp.int32),
        ),
        in_specs=[smem, anywhere, anywhere, anywhere],
        out_specs=(pl.BlockSpec(memory_space=pltpu.VMEM), anywhere, anywhere, anywhere, smem),
        scratch_shapes=[
            pltpu.VMEM((tasks - SPREAD,) + meta.shape, meta.dtype),
            pltpu.VMEM(ao_tiles.shape, ao_tiles.dtype),
            pltpu.VMEM(shares, ao_tiles.dtype),
            dma((tasks - 1,)),
            dma((tasks - 1,)),
            dma((chips,)),
            dma((chips,)),
            dma((chips,)),
            dma((chips,)),
            dma((SPREAD - 1,)),
            dma((SPREAD - 1,)),
            dma((2,)),
            dma((8 if tiles % 8 == 0 else 1,)),
            dma((5 if rows % 5 == 0 else 2,)),
        ],
        compiler_params=pltpu.CompilerParams(
            collective_id=0, has_side_effects=True, vmem_limit_bytes=66 * 1000 * 1000
        ),
        name="exchange",
    )(slots, meta, coeff, ao_tiles)


def work_kernel(tasks, occs, nu_range, chunks, step, ratio, near_ref, slots_ref, tiles, packed, early, coeffs, total, *refs):
    recv, held, flat, spread_rows, coeff_i, left_a, left_b, lhs_a, lhs_b, stage, mixed, mu_rows = refs[:12]
    taken, kept, on, oned, over, overed, side, sided = refs[12:]
    place = Place(tasks, occs)
    count, mu_width, nu_width, kl = tiles.shape
    all_occ, tall = total.shape[:2]
    occ = coeffs.shape[1]
    room = list_room(count)
    meta = near_ref.shape[0] // SPREAD
    counts_at = SPREAD * room
    per = LANES // nu_width
    lists = range(SPREAD - 1)
    hopses = range(1, place.chips)
    own_steps = own_steps_of(chunks)
    ticks, size = chunks * ratio, step // ratio

    parts = taken.shape[0]
    part = count // parts
    takes = [
        pltpu.make_async_copy(tiles.at[pl.ds(k * part, part)], held.at[pl.ds(k * part, part)], taken.at[k])
        for k in range(parts)
    ]

    def onward(s, k):
        return send(
            packed.at[s, pl.ds(k * size, size)],
            recv.at[s, place.me, pl.ds(k * size, size)],
            (on.at[s, k], oned.at[s, k]),
            place.ahead(s + 1),
        )

    def cross(s, k, hops):
        block = recv.at[s, place.me, pl.ds(k * size, size)]
        return send(block, block, (over.at[s, k, hops - 1], overed.at[s, k, hops - 1]), place.across(hops))

    def aside(s, k, hops):
        block = recv.at[s, place.across_index(-hops), pl.ds(k * size, size)]
        return send(block, block, (side.at[s, k, hops], sided.at[s, k, hops]), place.sibling())

    def loop(upper, act):
        def body(k, carry):
            act(k)
            return carry

        lax.fori_loop(0, upper, body, 0)

    def clear(ref, pieces):
        size = ref.shape[0] // pieces

        def body(k):
            ref[pl.ds(k * size, size)] = jnp.zeros((size,) + ref.shape[1:], ref.dtype)

        loop(pieces, body)

    keeps = [pltpu.make_async_copy(early.at[s], recv.at[s, place.me, pl.ds(0, step)], kept.at[s]) for s in lists]

    def launch(k):
        for s in lists:
            onward(s, k).start()

    def spread(k, came=None):
        for s in lists:
            (came or (lambda s: onward(s, k).wait_recv()))(s)
            for hops in hopses:
                cross(s, k, hops).start()
            aside(s, k, 0).start()

    def relay(k):
        for s in lists:
            for hops in hopses:
                cross(s, k, hops).wait_recv()
                aside(s, k, hops).start()

    for copy in keeps + takes:
        copy.start()
    clear(left_a.at[0], 16)
    clear(left_a.at[1], 16)
    place.greet((1, 2, tasks - 1, tasks - 2))
    lax.fori_loop(ratio, ticks, lambda k, carry: (launch(k), carry)[1], 0)
    for copy in keeps:
        copy.wait()
    for k in range(ratio):
        spread(k, lambda s: None)
    clear(left_b.at[0], 16)
    clear(left_b.at[1], 16)
    clear(total, 20)
    turn = (((0,), (0,)), ((), ()))
    unit = (
        lax.broadcasted_iota(jnp.int32, (tall, occ), 0) == lax.broadcasted_iota(jnp.int32, (tall, occ), 1)
    ).astype(F32).astype(BF16)
    rows_i = lax.dot_general(coeffs[place.me], unit[:occ], turn, preferred_element_type=F32)
    coeff_i[...] = rows_i.reshape(coeff_i.shape)
    for q in range(occs):
        flat[q * occ : (q + 1) * occ, :] = coeffs[q].astype(F32)
    source = lax.broadcasted_iota(jnp.int32, (LANES, per * LANES), 0)
    column = lax.broadcasted_iota(jnp.int32, (LANES, per * LANES), 1)
    repeat = (source == column // LANES * nu_width + column % nu_width).astype(F32).astype(BF16)

    def lay(c, carry):
        block = flat[:, pl.ds(pl.multiple_of(c * LANES, LANES), LANES)].astype(BF16)
        got = jnp.dot(block, repeat, preferred_element_type=F32)
        for r in range(per):
            spread_rows[c * per + r] = got[:, r * LANES : (r + 1) * LANES]
        return carry

    lax.fori_loop(0, flat.shape[1] // LANES, lay, 0, unroll=4)

    lane = lax.broadcasted_iota(jnp.int32, (1, LANES), 1) // nu_width
    band = all_occ // 4
    width = mu_width * GROUP
    steps = own_steps + chunks
    far_off = steps + own_steps + 1

    def counted(s):
        return near_ref[s * meta + counts_at + s]

    def list_of(e, g):
        j = (e + far_off - own_steps) // far_off
        own, c = e * 2 * GROUP + g * GROUP, (e - own_steps) * GROUP
        base = (1 - j) * own + j * ((g + 1) * (meta + room) + c)
        return base, (1 - j) * (counted(0) - own) + j * (counted(g + 1) - c)

    def build(e, g, left, lhs):
        base, valid = list_of(e, g)
        for b in range(GROUP):
            live = jnp.where(b < valid, 1.0, 0.0)
            mask = jnp.where(lane == b % per, live, 0.0)
            nu = lax.rem(near_ref[base + b], nu_range)
            left[b // per, pl.ds(b, all_occ, stride=GROUP), :] = spread_rows[nu] * mask
        for h in range(GROUP // per):
            lhs[:, h * LANES : (h + 1) * LANES] = left[h].astype(BF16)

    def first(g, lhs):
        for p in range(mu_width // 2):
            halves = [stage[g * GROUP : (g + 1) * GROUP, m].reshape(GROUP * nu_width, kl) for m in (2 * p, 2 * p + 1)]
            rhs = jnp.concatenate(halves, axis=1)
            at = g * width + 2 * p * GROUP
            for r in range(4):
                got = jnp.dot(
                    lhs[r * band * GROUP : (r + 1) * band * GROUP, :], rhs, preferred_element_type=F32
                ).reshape(band, GROUP, 2 * kl)
                got = jnp.concatenate([got[:, :, :kl], got[:, :, kl:]], axis=1)
                mixed[r * band : (r + 1) * band, at : at + 2 * GROUP, :] = got.astype(BF16)

    def second(e):
        for g in range(2):
            base = list_of(e, g)[0]
            for b in range(GROUP):
                mu = lax.div(near_ref[base + b], nu_range)
                mu_rows[pl.ds(g * width + b, mu_width, stride=GROUP), :] = coeff_i[mu]
        left_i = lax.dot_general(
            unit, mu_rows[...].astype(BF16), (((1,), (1,)), ((), ())), preferred_element_type=F32
        ).astype(BF16)
        for j in range(0, all_occ, 2):
            both = jnp.concatenate([mixed[j], mixed[j + 1]], axis=1)
            got = jnp.dot(left_i, both, preferred_element_type=F32)
            total[j] += got[:, :kl]
            total[j + 1] += got[:, kl:]

    build(0, 0, left_a, lhs_a)
    for take in takes:
        take.wait()
    def within(tick, act, least=0):
        @pl.when(tick >= least)
        def _():
            @pl.when(tick < ticks)
            def _():
                act(tick)

    def take_step(e):
        c = e - own_steps

        @pl.when(c < 0)
        def _():
            @pl.when(e == 1)
            def _():
                spread(1)
                relay(0)

            @pl.when(c == -1)
            def _():
                spread(2)

            for b in range(2 * GROUP):
                stage[b] = held[slots_ref[e * 2 * GROUP + b]]

        @pl.when(c >= 0)
        def _():
            within(c + 2, spread, 3)
            for s in lists:
                for d in range(ratio):
                    for hops in range(place.chips):
                        aside(s, c * ratio + d, hops).wait_recv()
                for b in range(GROUP):
                    stage[s * GROUP + b] = recv[s, b % occs, c * step + b // occs]

        build(e, 1, left_b, lhs_b)
        first(0, lhs_a)
        first(1, lhs_b)

        build(e + 1, 0, left_a, lhs_a)
        second(e)

        @pl.when(c == -1)
        def _():
            relay(1)

        @pl.when(c == 0)
        def _():
            relay(2)

        @pl.when(c >= 2)
        def _():
            within(c + 1, relay)

    loop(steps, take_step)

    def finish(k):
        @pl.when(k >= ratio)
        def _():
            for s in lists:
                onward(s, k).wait_send()

        for s in lists:
            for hops in hopses:
                cross(s, k, hops).wait_send()
            for hops in range(place.chips):
                aside(s, k, hops).wait_send()

    loop(ticks, finish)


def work(tasks, occs, nu_range, index, rows, step, near, slots, ao_tiles, packed, early, coeffs):
    anywhere = pl.BlockSpec(memory_space=pl.ANY)
    smem = pl.BlockSpec(memory_space=pltpu.SMEM)
    vmem = pltpu.VMEM
    chips = occs // 2
    chunks = rows // step
    ratio = 1
    ticks = chunks * ratio
    dma = pltpu.SemaphoreType.DMA
    lists = SPREAD - 1
    count, mu_width, nu_width, kl = ao_tiles.shape
    _, occ, basis = coeffs.shape
    all_occ, tall = occs * occ, up(occ, 8)
    depth = 2 * GROUP * mu_width
    return pl.pallas_call(
        partial(work_kernel, tasks, occs, nu_range, chunks, step, ratio),
        out_shape=jax.ShapeDtypeStruct((all_occ, tall, kl), F32),
        in_specs=[smem, smem, anywhere, anywhere, anywhere, pl.BlockSpec(memory_space=pltpu.VMEM)],
        out_specs=pl.BlockSpec(memory_space=pltpu.VMEM),
        scratch_shapes=[
            vmem((lists, occs, rows) + ao_tiles.shape[1:], BF16),
            vmem(ao_tiles.shape, BF16),
            vmem((all_occ, basis), F32),
            vmem((nu_range, all_occ, LANES), F32),
            vmem((basis // mu_width, mu_width, occ), F32),
            vmem((GROUP * nu_width // LANES, all_occ * GROUP, LANES), F32),
            vmem((GROUP * nu_width // LANES, all_occ * GROUP, LANES), F32),
            vmem((all_occ * GROUP, GROUP * nu_width), BF16),
            vmem((all_occ * GROUP, GROUP * nu_width), BF16),
            vmem((2 * GROUP,) + ao_tiles.shape[1:], BF16),
            vmem((all_occ, depth, kl), BF16),
            vmem((depth, occ), F32),
            dma((8 if count % 8 == 0 else 1,)),
            dma((lists,)),
            dma((lists, ticks)),
            dma((lists, ticks)),
            dma((lists, ticks, chips)),
            dma((lists, ticks, chips)),
            dma((lists, ticks, chips)),
            dma((lists, ticks, chips)),
        ],
        compiler_params=pltpu.CompilerParams(
            collective_id=1 + index, has_side_effects=True, vmem_limit_bytes=66 * 1000 * 1000
        ),
        name="work" + str(rows),
    )(near, slots, ao_tiles, packed, early, coeffs)


def turn_kernel(turned, out, held, made, taken, put):
    parts, _, rows, kl = held.shape
    kept = out.shape[0]
    takes = [
        pltpu.make_async_copy(turned.at[:, pl.ds(p * rows, rows)], held.at[p], taken.at[p]) for p in range(parts)
    ]
    for take in takes:
        take.start()
    puts = []
    for p in range(parts):
        takes[p].wait()
        have = min(rows, kept - p * rows)
        block = held[p]
        for i in range(have):
            made[p * rows + i] = block[:, i, :]
        puts.append(
            pltpu.make_async_copy(made.at[pl.ds(p * rows, have)], out.at[pl.ds(p * rows, have)], put.at[p])
        )
        puts[-1].start()
    for copy in puts:
        copy.wait()


def turn_back(turned, occ):
    all_occ, tall, kl = turned.shape
    parts = tall // 8
    anywhere = pl.BlockSpec(memory_space=pl.ANY)
    return pl.pallas_call(
        turn_kernel,
        out_shape=jax.ShapeDtypeStruct((occ, all_occ, kl), F32),
        in_specs=[anywhere],
        out_specs=anywhere,
        scratch_shapes=[
            pltpu.VMEM((parts, all_occ, 8, kl), F32),
            pltpu.VMEM((occ, all_occ, kl), F32),
            pltpu.SemaphoreType.DMA((parts,)),
            pltpu.SemaphoreType.DMA((parts,)),
        ],
        compiler_params=pltpu.CompilerParams(vmem_limit_bytes=48 * 1024 * 1024),
        name="turn",
    )(turned)


CLASSES = (6, 7, 8, 9, 10)


def local(ao_tiles, mo_coeffs, mu_blocks, nu_blocks, tile_live, batch_target, batch_count):
    tiles, _, nu_width, _ = ao_tiles.shape
    tasks, occs = lax.axis_size("task"), lax.axis_size("occ")
    nu_range = mo_coeffs.shape[0] // nu_width
    step = GROUP // occs
    rows = up(-(-tiles // occs), step)
    classes = [c * step for c in CLASSES if c * step < rows] + [rows]
    limits = [(r * occs, 2 * GROUP * own_steps_of(r // step)) for r in classes]
    coeff = mo_coeffs.T

    meta, slots = make_plan(nu_range, tile_live, batch_target, batch_count, mu_blocks, nu_blocks)
    near, coeffs, packed, early, picked = exchange(
        tasks, occs, rows, step, limits, slots, meta.reshape(-1, LANES), coeff, ao_tiles
    )
    branches = [partial(work, tasks, occs, nu_range, index, size, step) for index, size in enumerate(classes)]
    turned = lax.switch(picked[0], branches, near.reshape(-1), slots, ao_tiles, packed, early, coeffs)
    return turn_back(turned, coeff.shape[0])


def solution(mesh):
    in_specs = (
        P("task", None, None, None),
        P(None, "occ"),
        P("task"),
        P("task"),
        P("task"),
        P("task"),
        P("task"),
    )
    out_specs = P("occ", None, "task")
    return jax.shard_map(local, mesh=mesh, in_specs=in_specs, out_specs=out_specs, check_vma=False)
```
